32 devices in a mesh: gx: 2 (over y), gy: 4 (over z), lev: 4 (over x, core).
Axes of the slice: x: 2, y: 2, z: 4, core: 2. Of those that a mesh axis runs over, the one named last changes fastest.
Arguments:
- state: bfloat16 [256, 32, 8, 512], P('gx', 'gy', 'lev'), may hold values from -6 to 6
- obs_col: int32 [1024], P('gx'), may hold values from 0 to 127
- obs_row: int32 [1024], P('gx'), may hold values from 0 to 31
- foot_off: int32 [1024, 8], P('gx'), may hold values from 0 to 84
- obs_lev: int32 [1024], P('gx'), may hold values from 0 to 7
- obs_val: float32 [1024], P('gx'), may hold values from -6 to 6
- obs_err: float32 [1024], P('gx'), may hold values from 0.5 to 2
- loc: bfloat16 [256, 32, 512], P('gx', ('gy', 'lev')), may hold values from 0.099609375 to 1
Outputs:
- mean_out: float32 [256, 32, 8], P('gx', ('gy', 'lev'))
- anom_out: bfloat16 [256, 32, 8, 512], P('gx', ('gy', 'lev'))
The draws below stay inside these ranges and needn't reach their ends.
All inputs are finite; a program needn't handle non-finite values.
Results may differ from the reference program's by a relative error of at most 0.009.
Values may be sent and summed in bfloat16 or wider, within the bound.
A program may use at most 64 MiB of HBM per device.

```python
import math
import jax
import jax.numpy as jnp
from jax import lax

M = 512
CXD = 128
LEV = 8
NOBS = 512
KF = 8
HW = 8
DY = 2
NX = 256
NY = 32
OBS_ALL = 1024
N_GX = 2


def place_ends(entries, key, smallest, high):
    extent = entries.shape
    spot = [jax.random.randint(jax.random.fold_in(key, axis), (), 0, extent[axis]) for axis in range(len(extent))]
    entries = entries.at[tuple(spot)].set(smallest)
    longest = extent.index(max(extent))
    spot[longest] = (spot[longest] + 1) % extent[longest]
    return entries.at[tuple(spot)].set(high)


def block_levels(own_key, dims, pieces, smallest, top_value):
    level, own = 1.0, jax.random.fold_in(own_key, 6)
    for dim, parts in pieces:
        draws = jnp.exp(jax.random.uniform(jax.random.fold_in(own, dim), (parts,), jnp.float32, smallest / len(pieces), top_value / len(pieces)))
        level = level * jnp.repeat(draws, dims[dim] // parts).reshape([-1 if axis == dim else 1 for axis in range(len(dims))])
    return level


def gaussian(own_key, dims, deviation, most, shards=(), kind=jnp.bfloat16):
    level = block_levels(own_key, dims, shards, -0.22, 0.18) if shards else 1.0
    array = jax.random.normal(own_key, dims, jnp.float32) * deviation * level
    return jnp.minimum(jnp.maximum(array, -most), most).astype(kind)


def setup_inputs(seed: int = 0) -> dict:
    key_of = jax.random.split(jax.random.key(seed), 9)
    return {
        "state": gaussian(key_of[0], (NX, NY, LEV, M), 1.0, 6.0, ((0, 2), (1, 4), (2, 4))),
        "obs_col": place_ends(jax.random.randint(key_of[1], (OBS_ALL,), 0, CXD), jax.random.fold_in(key_of[1], 1), 0, CXD - 1).astype(jnp.int32),
        "obs_row": place_ends(jax.random.randint(key_of[2], (OBS_ALL,), 0, NY), jax.random.fold_in(key_of[2], 1), 0, NY - 1).astype(jnp.int32),
        "foot_off": place_ends(jax.random.randint(key_of[3], (OBS_ALL, KF), 0, (2 * HW + 1) * (2 * DY + 1)), jax.random.fold_in(key_of[3], 1), 0, ((2 * HW + 1) * (2 * DY + 1)) - 1).astype(jnp.int32),
        "obs_lev": place_ends(jax.random.randint(key_of[4], (OBS_ALL,), 0, LEV), jax.random.fold_in(key_of[4], 1), 0, LEV - 1).astype(jnp.int32),
        "obs_val": gaussian(key_of[5], (OBS_ALL,), 1.0, 6.0, ((0, 2),), jnp.float32),
        "obs_err": jnp.clip(jnp.exp(math.log(2.0) - 1.3862944 * jax.random.uniform(key_of[6], (OBS_ALL,), jnp.float32) ** block_levels(key_of[6], (OBS_ALL,), ((0, 2),), -0.2, 0.2)), 0.5, 2.0),
        "loc": jnp.clip(0.099609375 + 0.9003906 * jax.random.uniform(key_of[7], (NX, NY, NOBS), jnp.float32) ** block_levels(key_of[7], (NX, NY, NOBS), ((0, 2), (1, 16)), -0.2, 0.2), 0.099609375, 1.0).astype(jnp.bfloat16),
    }


def footprint(obs_col, obs_row, foot_off):
    span = 2 * DY + 1
    shift_x = foot_off // span - HW
    shift_y = foot_off % span - DY
    x_ext = obs_col[:, None] + shift_x + HW
    y_glob = jnp.clip(obs_row[:, None] + shift_y, 0, NY - 1)
    return (x_ext.astype(jnp.int32), y_glob.astype(jnp.int32))

def analyse(block, weight, hx_sum, values, errors):
    members = block.shape[-1]
    hbar = lax.optimization_barrier(jnp.mean(hx_sum, axis=1))
    yanom = hx_sum - hbar[:, None]
    innov = values - hbar
    cov = jnp.dot(yanom, yanom.T, precision=lax.Precision.HIGHEST) / (members - 1) + jnp.diag(errors)
    chol = jnp.linalg.cholesky(cov)
    root = chol + jnp.diag(jnp.sqrt(errors))
    first = lax.linalg.triangular_solve(chol, innov[:, None], left_side=True, lower=True)
    scaled = lax.linalg.triangular_solve(root, yanom, left_side=True, lower=True)
    wvec = lax.linalg.triangular_solve(chol, first, left_side=True, lower=True, transpose_a=True)[:, 0]
    zmat = lax.linalg.triangular_solve(chol, scaled, left_side=True, lower=True, transpose_a=True).astype(jnp.bfloat16)
    xbar = lax.optimization_barrier(jnp.mean(block, axis=-1, dtype=jnp.float32))
    anom = (block.astype(jnp.float32) - xbar[..., None]).astype(jnp.bfloat16)
    flat = anom.reshape(-1, members)
    cross = jnp.dot(flat.astype(jnp.float32), yanom.astype(jnp.bfloat16).T.astype(jnp.float32), preferred_element_type=jnp.float32) / (members - 1)
    n_obs = hx_sum.shape[0]
    gain = (cross.reshape(block.shape[:-1] + (n_obs,)) * weight[:, :, None, :].astype(jnp.float32)).astype(jnp.bfloat16)
    mean_part = xbar + lax.optimization_barrier(jnp.sum(gain.astype(jnp.float32) * wvec, axis=-1))
    update = jnp.dot(gain.reshape(-1, n_obs).astype(jnp.float32), zmat.astype(jnp.float32), preferred_element_type=jnp.float32)
    anom_part = (flat.astype(jnp.float32) - update).astype(jnp.bfloat16).reshape(block.shape)
    return (mean_part, anom_part)

def reference(state, obs_col, obs_row, foot_off, obs_lev, obs_val, obs_err, loc):

    def one_tile(inputs):
        index, cols, rows, offsets, levels, values, errors = inputs
        x_ext, y_glob = footprint(cols, rows, offsets)
        x_glob = ((index * CXD + x_ext - HW) % NX).astype(jnp.int32)
        picked = state[x_glob, y_glob, levels[:, None].astype(jnp.int32), :]
        hx_sum = lax.optimization_barrier(jnp.sum(picked.astype(jnp.float32), axis=1)) / KF
        block = lax.dynamic_slice_in_dim(state, (index * CXD).astype(jnp.int32), CXD, 0)
        weight = lax.dynamic_slice_in_dim(loc, (index * CXD).astype(jnp.int32), CXD, 0)
        return analyse(block, weight, hx_sum, values, errors)
    tiles = (jnp.arange(N_GX, dtype=jnp.int32), obs_col.reshape(N_GX, NOBS), obs_row.reshape(N_GX, NOBS), foot_off.reshape(N_GX, NOBS, KF), obs_lev.reshape(N_GX, NOBS), obs_val.reshape(N_GX, NOBS), obs_err.reshape(N_GX, NOBS))
    means, anoms = lax.map(one_tile, tiles)
    return (means.reshape(NX, NY, LEV), anoms.reshape(NX, NY, LEV, M))
```

```python
import jax
import jax.numpy as jnp
from jax import lax
from jax.experimental import pallas as pl
from jax.experimental.pallas import tpu as pltpu
from jax.sharding import PartitionSpec as P

KF = 8
HW = 8
DY = 2
SUB = 8
LANES = 128
BLOCK = 64


def padded_2(array, sides, width):
    for axis, dim in sides:
        size, length = (lax.axis_size(axis), array.shape[dim])
        up = [(i, (i + 1) % size) for i in range(size)]
        down = [(j, i) for i, j in up]
        last = lax.slice_in_dim(array, length - width, length, axis=dim)
        first = lax.slice_in_dim(array, 0, width, axis=dim)
        before = lax.ppermute(last, axis, up)
        after = lax.ppermute(first, axis, down)
        array = jnp.concatenate([before, array, after], axis=dim)
    return array


def footprint_code(obs_col, obs_row, foot_off, ny_total):
    span = 2 * DY + 1
    shift_x = foot_off // span - HW
    shift_y = foot_off % span - DY
    x_ext = obs_col[:, None] + shift_x + HW
    y_glob = jnp.clip(obs_row[:, None] + shift_y, 0, ny_total - 1)
    return x_ext * ny_total + y_glob


def observe(block, y_start, foot_code, obs_lev, ny_total):
    padded = padded_2(block, (("gx", 0),), HW)
    ext_x, y_count, lev_count, members = padded.shape
    col_id = (
        jnp.arange(ext_x, dtype=jnp.int32)[:, None] * ny_total
        + y_start
        + jnp.arange(y_count, dtype=jnp.int32)[None, :]
    ).reshape(-1)
    n_obs = foot_code.shape[0]
    hit_count = jnp.zeros((n_obs, col_id.shape[0]), jnp.float32)
    for slot in range(foot_code.shape[1]):
        hit_count = hit_count + (foot_code[:, slot, None] == col_id[None, :]).astype(jnp.float32)
    level_hit = (obs_lev[:, None] == jnp.arange(lev_count, dtype=jnp.int32)[None, :]).astype(
        jnp.float32
    )
    select = (hit_count[:, :, None] * level_hit[:, None, :]).reshape(n_obs, -1).astype(jnp.bfloat16)
    return jnp.dot(select, padded.reshape(-1, members), preferred_element_type=jnp.float32)


def relay(state):
    return lax.all_to_all(state, "lev", split_axis=1, concat_axis=2, tiled=True)


def lane_cast(value, k):
    return jnp.broadcast_to(value[:, k : k + 1], value.shape)


def row_cast(value, i):
    return jnp.broadcast_to(value[i : i + 1, :], value.shape)


def f32_dot(a, b, dims):
    return lax.dot_general(
        a, b, (dims, ((), ())), precision=lax.Precision.HIGHEST, preferred_element_type=jnp.float32
    )


def factor_block(w_ref, x_ref, root_err):
    rows = w_ref.shape[0]
    groups = rows // SUB
    w = [w_ref[SUB * g : SUB * (g + 1), :] for g in range(groups)]
    x = [x_ref[SUB * g : SUB * (g + 1), :] for g in range(groups)]
    sub_id = lax.broadcasted_iota(jnp.int32, (SUB, LANES), 0)
    for g in range(groups):
        col = {h: [lane_cast(w[h], SUB * g + m) for m in range(SUB)] for h in range(g, groups)}
        s = {(i, m): row_cast(col[g][m], i) for m in range(SUB) for i in range(m, SUB)}
        wr = [row_cast(w[g], i) for i in range(SUB)]
        xr = [row_cast(x[g], i) for i in range(SUB)]
        inv = []
        for k in range(SUB):
            pivot = s[k, k]
            inv_k = lax.rsqrt(pivot)
            inv.append(inv_k)
            minv_k = 1.0 / (pivot * inv_k + row_cast(root_err[g], k))
            for i in range(k + 1, SUB):
                s[i, k] = s[i, k] * inv_k
            for m in range(k + 1, SUB):
                for i in range(m, SUB):
                    s[i, m] = s[i, m] - s[i, k] * s[m, k]
            wr[k] = wr[k] * inv_k
            xr[k] = xr[k] * minv_k
            for i in range(k + 1, SUB):
                wr[i] = wr[i] - s[i, k] * wr[k]
                xr[i] = xr[i] - s[i, k] * xr[k]
        w_new, x_new = wr[0], xr[0]
        for k in range(1, SUB):
            w_new = jnp.where(sub_id == k, wr[k], w_new)
            x_new = jnp.where(sub_id == k, xr[k], x_new)
        w[g], x[g] = w_new, x_new
        for k in reversed(range(SUB)):
            wr[k] = wr[k] * inv[k]
            xr[k] = xr[k] * inv[k]
            for i in range(k):
                wr[i] = wr[i] - s[k, i] * wr[k]
                xr[i] = xr[i] - s[k, i] * xr[k]
        for h in range(g + 1, groups):
            for m in range(SUB):
                w[h] = w[h] - col[h][m] * wr[m]
                x[h] = x[h] - col[h][m] * xr[m]
    for g in range(groups):
        w_ref[SUB * g : SUB * (g + 1), :] = w[g]
        x_ref[SUB * g : SUB * (g + 1), :] = x[g]


def weights_kernel(hx_ref, val_ref, err_ref, z_ref, w_out_ref, y_ref, a_ref, s_ref, root_ref, w_ref, x_ref, inv_ref, low_ref):
    n, members = hx_ref.shape
    blocks = n // BLOCK
    hx = hx_ref[...]
    hbar = jnp.mean(hx, axis=1, keepdims=True)
    yanom = hx - hbar
    y_ref[...] = yanom.astype(jnp.bfloat16)
    s_ref[:, :members] = yanom
    s_ref[:, members:] = jnp.broadcast_to(val_ref[...] - hbar, (n, LANES))
    root_ref[...] = jnp.broadcast_to(jnp.sqrt(err_ref[...]), (n, LANES))
    same = lax.broadcasted_iota(jnp.int32, (n, n), 0) == lax.broadcasted_iota(jnp.int32, (n, n), 1)
    a_ref[...] = f32_dot(yanom, yanom, ((1,), (1,))) / (members - 1) + jnp.where(same, err_ref[...], 0.0)
    eye_w = lax.broadcasted_iota(jnp.int32, (BLOCK, LANES), 0) + BLOCK == lax.broadcasted_iota(jnp.int32, (BLOCK, LANES), 1)
    eye_x = lax.broadcasted_iota(jnp.int32, (BLOCK, LANES), 0) == lax.broadcasted_iota(jnp.int32, (BLOCK, LANES), 1)

    def load_block(at):
        w_ref[...] = jnp.where(eye_w, 1.0, 0.0)
        w_ref[:, :BLOCK] = a_ref[at : at + BLOCK, at : at + BLOCK]
        x_ref[...] = jnp.where(eye_x, 1.0, 0.0)

    load_block(0)

    def step(k, carry):
        base = pl.multiple_of(k * BLOCK, BLOCK)
        root_err = [root_ref[pl.ds(base + SUB * g, SUB), :] for g in range(BLOCK // SUB)]
        factor_block(w_ref, x_ref, root_err)
        for kk in range(blocks):

            @pl.when(k == kk)
            def _():
                at, end = kk * BLOCK, (kk + 1) * BLOCK
                l_inv = w_ref[:, BLOCK:]
                m_inv = x_ref[:, :BLOCK]
                inv_ref[kk] = l_inv
                s_ref[at:end, :members] = f32_dot(m_inv, s_ref[at:end, :members], ((1,), (0,)))
                s_ref[at:end, members:] = f32_dot(l_inv, s_ref[at:end, members:], ((1,), (0,)))
                if end < n:
                    left = end // LANES * LANES
                    panel = f32_dot(a_ref[left:, at:end], l_inv, ((1,), (1,)))
                    below = panel[end - left :]
                    low_ref[kk, end:, :] = below
                    a_ref[end:, left:] = a_ref[end:, left:] - f32_dot(below, panel, ((1,), (1,)))
                    load_block(end)
                    s_ref[end:, :] = s_ref[end:, :] - f32_dot(below, s_ref[at:end, :], ((1,), (0,)))

        return carry

    lax.fori_loop(0, blocks, step, 0)
    for kk in reversed(range(blocks)):
        at, end = kk * BLOCK, (kk + 1) * BLOCK
        right = s_ref[at:end, :]
        if end < n:
            right = right - f32_dot(low_ref[kk, end:, :], s_ref[end:, :], ((0,), (0,)))
        s_ref[at:end, :] = f32_dot(inv_ref[kk], right, ((0,), (0,)))
    z_ref[...] = s_ref[:, :members].astype(jnp.bfloat16)
    w_out_ref[...] = s_ref[:, members:]


def weights(hx, values, errors):
    n, members = hx.shape
    return pl.pallas_call(
        weights_kernel,
        name="weights",
        out_shape=(
            jax.ShapeDtypeStruct((n, members), jnp.bfloat16),
            jax.ShapeDtypeStruct((n, LANES), jnp.float32),
            jax.ShapeDtypeStruct((n, members), jnp.bfloat16),
        ),
        in_specs=[pl.BlockSpec(memory_space=pltpu.VMEM)] * 3,
        out_specs=tuple([pl.BlockSpec(memory_space=pltpu.VMEM)] * 3),
        scratch_shapes=[
            pltpu.VMEM((n, n), jnp.float32),
            pltpu.VMEM((n, members + LANES), jnp.float32),
            pltpu.VMEM((n, LANES), jnp.float32),
            pltpu.VMEM((BLOCK, LANES), jnp.float32),
            pltpu.VMEM((BLOCK, LANES), jnp.float32),
            pltpu.VMEM((n // BLOCK, BLOCK, BLOCK), jnp.float32),
            pltpu.VMEM((n // BLOCK, n, BLOCK), jnp.float32),
        ],
        compiler_params=pltpu.CompilerParams(vmem_limit_bytes=48 * 1024 * 1024),
    )(hx, values[:, None], errors[:, None])


def analyse(block, weight, hx_sum, values, errors):
    members = block.shape[-1]
    zmat, wcol, ybf = weights(hx_sum, values, errors)
    wvec = wcol[:, 0]
    xbar = jnp.mean(block, axis=-1, dtype=jnp.float32)
    anom = (block.astype(jnp.float32) - xbar[..., None]).astype(jnp.bfloat16)
    flat = anom.reshape(-1, members)
    cross = jnp.dot(flat, ybf.T, preferred_element_type=jnp.float32) / (
        members - 1
    )
    n_obs = hx_sum.shape[0]
    gain = (
        cross.reshape(block.shape[:-1] + (n_obs,)) * weight[:, :, None, :].astype(jnp.float32)
    ).astype(jnp.bfloat16)
    mean_part = xbar + jnp.sum(gain.astype(jnp.float32) * wvec, axis=-1)
    update = jnp.dot(gain.reshape(-1, n_obs), zmat, preferred_element_type=jnp.float32)
    anom_part = (flat.astype(jnp.float32) - update).astype(jnp.bfloat16).reshape(block.shape)
    return (mean_part, anom_part)


def local(state, obs_col, obs_row, foot_off, obs_lev, obs_val, obs_err, loc):
    level_groups = lax.axis_size("lev")
    ny_total = loc.shape[1] * lax.axis_size("gy") * level_groups
    foot_code = footprint_code(obs_col, obs_row, foot_off, ny_total)
    y_block = loc.shape[1]
    relaid = relay(state)
    y_start = (lax.axis_index("gy") * level_groups + lax.axis_index("lev")) * y_block
    partial_sum = observe(relaid, y_start, foot_code, obs_lev, ny_total)
    hx_sum = lax.psum(partial_sum, ("gy", "lev")) / KF
    return analyse(relaid, loc, hx_sum, obs_val, obs_err)


def solution(mesh):
    return jax.shard_map(
        local,
        mesh=mesh,
        in_specs=(
            P("gx", "gy", "lev", None),
            P("gx"),
            P("gx"),
            P("gx", None),
            P("gx"),
            P("gx"),
            P("gx"),
            P("gx", ("gy", "lev"), None),
        ),
        out_specs=(P("gx", ("gy", "lev"), None), P("gx", ("gy", "lev"), None, None)),
        check_vma=False,
    )
```

```python
import functools

import jax
import jax.numpy as jnp
from jax import lax
from jax.experimental import pallas as pl
from jax.experimental.pallas import tpu as pltpu
from jax.sharding import PartitionSpec as P

KF = 8
HW = 8
DY = 2
SUB = 8
LANES = 128
BLOCK = 64
MESH = pl.DeviceIdType.MESH


def footprint_code(obs_col, obs_row, foot_off, obs_lev, shape, ny_total, y_start, lev_start):
    y_count, lev_count = shape
    span = 2 * DY + 1
    shift_x = foot_off // span - HW
    shift_y = foot_off % span - DY
    x_ext = obs_col[:, None] + shift_x + HW
    y_here = jnp.clip(obs_row[:, None] + shift_y, 0, ny_total - 1) - y_start
    lev_here = obs_lev[:, None] - lev_start
    inside = (y_here >= 0) & (y_here < y_count) & (lev_here >= 0) & (lev_here < lev_count)
    return jnp.where(inside, (x_ext * y_count + y_here) * lev_count + lev_here, -1)


def lane_cast(value, k):
    return jnp.broadcast_to(value[:, k : k + 1], value.shape)


def row_cast(value, i):
    return jnp.broadcast_to(value[i : i + 1, :], value.shape)


def f32_dot(a, b, dims):
    return lax.dot_general(
        a, b, (dims, ((), ())), precision=lax.Precision.HIGHEST, preferred_element_type=jnp.float32
    )


def factor_block(w_ref, x_ref, root_err):
    rows = w_ref.shape[0]
    groups = rows // SUB
    w = [w_ref[SUB * g : SUB * (g + 1), :] for g in range(groups)]
    x = [x_ref[SUB * g : SUB * (g + 1), :] for g in range(groups)]
    sub_id = lax.broadcasted_iota(jnp.int32, (SUB, LANES), 0)
    for g in range(groups):
        col = {h: [lane_cast(w[h], SUB * g + m) for m in range(SUB)] for h in range(g, groups)}
        s = {(i, m): row_cast(col[g][m], i) for m in range(SUB) for i in range(m, SUB)}
        wr = [row_cast(w[g], i) for i in range(SUB)]
        xr = [row_cast(x[g], i) for i in range(SUB)]
        inv = []
        for k in range(SUB):
            pivot = s[k, k]
            inv_k = lax.rsqrt(pivot)
            inv.append(inv_k)
            minv_k = 1.0 / (pivot * inv_k + row_cast(root_err[g], k))
            for i in range(k + 1, SUB):
                s[i, k] = s[i, k] * inv_k
            for m in range(k + 1, SUB):
                for i in range(m, SUB):
                    s[i, m] = s[i, m] - s[i, k] * s[m, k]
            wr[k] = wr[k] * inv_k
            xr[k] = xr[k] * minv_k
            for i in range(k + 1, SUB):
                wr[i] = wr[i] - s[i, k] * wr[k]
                xr[i] = xr[i] - s[i, k] * xr[k]
        w_new, x_new = wr[0], xr[0]
        for k in range(1, SUB):
            w_new = jnp.where(sub_id == k, wr[k], w_new)
            x_new = jnp.where(sub_id == k, xr[k], x_new)
        w[g], x[g] = w_new, x_new
        for k in reversed(range(SUB)):
            wr[k] = wr[k] * inv[k]
            xr[k] = xr[k] * inv[k]
            for i in range(k):
                wr[i] = wr[i] - s[k, i] * wr[k]
                xr[i] = xr[i] - s[k, i] * xr[k]
        for h in range(g + 1, groups):
            for m in range(SUB):
                w[h] = w[h] - col[h][m] * wr[m]
                x[h] = x[h] - col[h][m] * xr[m]
    for g in range(groups):
        w_ref[SUB * g : SUB * (g + 1), :] = w[g]
        x_ref[SUB * g : SUB * (g + 1), :] = x[g]


def solve_weights(err_ref, z_ref, w_out_ref, y_ref, a_ref, s_ref, root_ref, w_ref, x_ref, inv_ref, low_ref):
    n, members = y_ref.shape
    blocks = n // BLOCK
    ybf = s_ref[:, :members].astype(jnp.bfloat16)
    y_ref[...] = ybf
    root_ref[...] = jnp.broadcast_to(jnp.sqrt(err_ref[...]), (n, LANES))
    same = lax.broadcasted_iota(jnp.int32, (n, n), 0) == lax.broadcasted_iota(jnp.int32, (n, n), 1)
    a_ref[...] = lax.dot_general(ybf, ybf, (((1,), (1,)), ((), ())), preferred_element_type=jnp.float32) / (members - 1) + jnp.where(same, err_ref[...], 0.0)
    eye_w = lax.broadcasted_iota(jnp.int32, (BLOCK, LANES), 0) + BLOCK == lax.broadcasted_iota(jnp.int32, (BLOCK, LANES), 1)
    eye_x = lax.broadcasted_iota(jnp.int32, (BLOCK, LANES), 0) == lax.broadcasted_iota(jnp.int32, (BLOCK, LANES), 1)

    def load_block(at):
        w_ref[...] = jnp.where(eye_w, 1.0, 0.0)
        w_ref[:, :BLOCK] = a_ref[at : at + BLOCK, at : at + BLOCK]
        x_ref[...] = jnp.where(eye_x, 1.0, 0.0)

    load_block(0)

    def step(k, carry):
        base = pl.multiple_of(k * BLOCK, BLOCK)
        root_err = [root_ref[pl.ds(base + SUB * g, SUB), :] for g in range(BLOCK // SUB)]
        factor_block(w_ref, x_ref, root_err)
        for kk in range(blocks):

            @pl.when(k == kk)
            def _():
                at, end = kk * BLOCK, (kk + 1) * BLOCK
                l_inv = w_ref[:, BLOCK:]
                m_inv = x_ref[:, :BLOCK]
                inv_ref[kk] = l_inv
                s_ref[at:end, :members] = f32_dot(m_inv, s_ref[at:end, :members], ((1,), (0,)))
                s_ref[at:end, members:] = f32_dot(l_inv, s_ref[at:end, members:], ((1,), (0,)))
                if end < n:
                    left = end // LANES * LANES
                    panel = f32_dot(a_ref[left:, at:end], l_inv, ((1,), (1,)))
                    below = panel[end - left :]
                    low_ref[kk, end:, :] = below
                    a_ref[end:, left:] = a_ref[end:, left:] - f32_dot(below, panel, ((1,), (1,)))
                    load_block(end)
                    s_ref[end:, :] = s_ref[end:, :] - f32_dot(below, s_ref[at:end, :], ((1,), (0,)))

        return carry

    lax.fori_loop(0, blocks, step, 0)
    for kk in reversed(range(blocks)):
        at, end = kk * BLOCK, (kk + 1) * BLOCK
        right = s_ref[at:end, :]
        if end < n:
            right = right - f32_dot(low_ref[kk, end:, :], s_ref[end:, :], ((0,), (0,)))
        s_ref[at:end, :] = f32_dot(inv_ref[kk], right, ((0,), (0,)))
    z_ref[...] = s_ref[:, :members].astype(jnp.bfloat16)
    w_out_ref[...] = s_ref[:, members:]


def analysis_weights_kernel(
    axes, code_ref, state_ref, raw_ref, val_ref, err_ref, z_ref, w_out_ref, y_ref, relaid_ref,
    acc_ref, before_ref, after_ref, zin_ref, ys_ref, hb_ref, half_refs,
    a_ref, s_ref, root_ref, w_ref, x_ref, inv_ref, low_ref, send_sem, recv_sem, own_sem,
):
    gxs, gys, levs = axes
    gx, gy, lev = lax.axis_index("gx"), lax.axis_index("gy"), lax.axis_index("lev")
    n, members = acc_ref.shape
    edge = before_ref.shape[0]
    inner = state_ref.shape[0]
    right, left = lax.rem(gx + 1, gxs), lax.rem(gx + gxs - 1, gxs)
    levels = [(lax.rem(lev + d, levs)) for d in range(1, levs)]
    lats = [(lax.rem(gy + d, gys)) for d in range(1, gys)]
    barrier = pltpu.get_barrier_semaphore()
    peers = [{"gx": right}, {"gx": left}] + [{"lev": v} for v in levels] + [{"gy": v} for v in lats]
    for peer in peers:
        pl.semaphore_signal(barrier, inc=1, device_id=peer, device_id_type=MESH)
    pl.semaphore_wait(barrier, len(peers))
    count = [0]

    def remote(src, dst, peer):
        i = count[0]
        count[0] += 1
        return pltpu.make_async_remote_copy(
            src_ref=src, dst_ref=dst, send_sem=send_sem.at[i], recv_sem=recv_sem.at[i],
            device_id=peer, device_id_type=MESH,
        )

    halo = [
        remote(state_ref.at[inner - edge : inner], before_ref, {"gx": right}),
        remote(state_ref.at[0:edge], after_ref, {"gx": left}),
    ]
    for copy in halo:
        copy.start()
    y_block = relaid_ref.shape[2]
    own = pltpu.make_async_copy(raw_ref.at[:, pl.ds(lev * y_block, y_block)], relaid_ref.at[lev], own_sem.at[0])
    own.start()

    def chosen(base, width):
        spot = lax.broadcasted_iota(jnp.int32, (n, width), 1) + base
        hits = jnp.zeros((n, width), jnp.float32)
        for slot in range(KF):
            hits = hits + jnp.where(code_ref[:, slot : slot + 1] == spot, 1.0, 0.0)
        return hits.astype(jnp.bfloat16)

    acc_ref[...] = jnp.zeros_like(acc_ref)
    width = 256

    def pick(i, carry):
        at = pl.multiple_of(i * width, width)
        acc_ref[...] += jnp.dot(
            chosen(edge + at, width), state_ref[pl.ds(at, width), :], preferred_element_type=jnp.float32
        )
        return carry

    lax.fori_loop(0, inner // width, pick, 0)
    sel_before, sel_after = chosen(0, edge), chosen(edge + inner, edge)
    for copy in halo:
        copy.wait()
    acc_ref[...] += jnp.dot(sel_before, before_ref[...], preferred_element_type=jnp.float32) + jnp.dot(
        sel_after, after_ref[...], preferred_element_type=jnp.float32
    )
    base, size = 0, n
    bits = levs.bit_length() - 1
    bases = []
    for b in range(bits):
        size //= 2
        bit = lax.rem(lev // (1 << b), 2)
        partner = lev + (1 - 2 * bit) * (1 << b)
        keep, give = base + bit * size, base + (1 - bit) * size
        copy = remote(acc_ref.at[pl.ds(pl.multiple_of(give, 8), size)], half_refs[b], {"lev": partner})
        copy.start()
        copy.wait()
        rows = pl.ds(pl.multiple_of(keep, 8), size)
        acc_ref[rows, :] = acc_ref[rows, :] + half_refs[b][...]
        base = keep
        bases.append((base, size, partner))
    part = n // (levs * gys)
    copies = []
    for d, lat in enumerate(lats):
        copies.append(
            remote(acc_ref.at[pl.ds(pl.multiple_of(base + lat * part, 8), part)], zin_ref.at[d], {"gy": lat})
        )
    for copy in copies:
        copy.start()
    for copy in copies:
        copy.wait()
    mine = base + gy * part
    total = acc_ref[pl.ds(pl.multiple_of(mine, 8), part), :]
    for d in range(gys - 1):
        total = total + zin_ref[d]
    hx = total / KF
    hbar = jnp.mean(hx, axis=1, keepdims=True)
    chunk = base // part + gy
    ys_ref[chunk] = (hx - hbar).astype(jnp.bfloat16)
    hb_ref[chunk] = jnp.broadcast_to(hbar, (part, LANES))
    copies = []
    for lat in lats:
        copies.append(remote(ys_ref.at[chunk], ys_ref.at[chunk], {"gy": lat}))
        copies.append(remote(hb_ref.at[chunk], hb_ref.at[chunk], {"gy": lat}))
    for copy in copies:
        copy.start()
    for copy in copies:
        copy.wait()
    for start, size, partner in reversed(bases):
        span = pl.ds(start // part, size // part)
        copies = [
            remote(ys_ref.at[span], ys_ref.at[span], {"lev": partner}),
            remote(hb_ref.at[span], hb_ref.at[span], {"lev": partner}),
        ]
        for copy in copies:
            copy.start()
        for copy in copies:
            copy.wait()
    copies = [
        remote(raw_ref.at[:, pl.ds(v * y_block, y_block)], relaid_ref.at[lev], {"lev": v}) for v in levels
    ]
    for copy in copies:
        copy.start()
    for c in range(levs * gys):
        s_ref[c * part : (c + 1) * part, :members] = ys_ref[c].astype(jnp.float32)
        s_ref[c * part : (c + 1) * part, members:] = val_ref[c * part : (c + 1) * part, :] - hb_ref[c]
    solve_weights(err_ref, z_ref, w_out_ref, y_ref, a_ref, s_ref, root_ref, w_ref, x_ref, inv_ref, low_ref)
    for copy in copies:
        copy.wait()
    own.wait()


def analysis_weights(state, code, values, errors):
    axes = tuple(lax.axis_size(name) for name in ("gx", "gy", "lev"))
    gxs, gys, levs = axes
    x_count, y_count, lev_count, members = state.shape
    n = values.shape[0]
    edge = HW * y_count * lev_count
    part = n // (gys * levs)
    bits = levs.bit_length() - 1
    copies = 2 + bits + (gys - 1) + 2 * (gys - 1) + 2 * bits + (levs - 1)
    vmem = pl.BlockSpec(memory_space=pltpu.VMEM)
    hbm = pl.BlockSpec(memory_space=pl.ANY)
    return pl.pallas_call(
        functools.partial(analysis_weights_kernel, axes),
        name="analysis_weights",
        out_shape=(
            jax.ShapeDtypeStruct((n, members), jnp.bfloat16),
            jax.ShapeDtypeStruct((n, LANES), jnp.float32),
            jax.ShapeDtypeStruct((n, members), jnp.bfloat16),
            jax.ShapeDtypeStruct((levs, x_count, y_count // levs, lev_count, members), jnp.bfloat16),
        ),
        in_specs=[vmem, vmem, hbm, vmem, vmem],
        out_specs=(vmem, vmem, vmem, hbm),
        scratch_shapes=[
            pltpu.VMEM((n, members), jnp.float32),
            pltpu.VMEM((edge, members), jnp.bfloat16),
            pltpu.VMEM((edge, members), jnp.bfloat16),
            pltpu.VMEM((gys - 1, part, members), jnp.float32),
            pltpu.VMEM((gys * levs, part, members), jnp.bfloat16),
            pltpu.VMEM((gys * levs, part, LANES), jnp.float32),
            [pltpu.VMEM((n >> (b + 1), members), jnp.float32) for b in range(bits)],
            pltpu.VMEM((n, n), jnp.float32),
            pltpu.VMEM((n, members + LANES), jnp.float32),
            pltpu.VMEM((n, LANES), jnp.float32),
            pltpu.VMEM((BLOCK, LANES), jnp.float32),
            pltpu.VMEM((BLOCK, LANES), jnp.float32),
            pltpu.VMEM((n // BLOCK, BLOCK, BLOCK), jnp.float32),
            pltpu.VMEM((n // BLOCK, n, BLOCK), jnp.float32),
            pltpu.SemaphoreType.DMA((copies,)),
            pltpu.SemaphoreType.DMA((copies,)),
            pltpu.SemaphoreType.DMA((1,)),
        ],
        compiler_params=pltpu.CompilerParams(
            collective_id=0, has_side_effects=True, vmem_limit_bytes=48 * 1024 * 1024
        ),
    )(code, state.reshape(-1, members), state, values[:, None], errors[:, None])


def analyse(block, weight, zmat, wvec, ybf):
    members = block.shape[-1]
    xbar = jnp.mean(block, axis=-1, dtype=jnp.float32)
    anom = (block.astype(jnp.float32) - xbar[..., None]).astype(jnp.bfloat16)
    flat = anom.reshape(-1, members)
    cross = jnp.dot(flat, ybf.T, preferred_element_type=jnp.float32) / (
        members - 1
    )
    n_obs = ybf.shape[0]
    gain = (
        cross.reshape(block.shape[:-1] + (n_obs,)) * weight[:, :, None, :].astype(jnp.float32)
    ).astype(jnp.bfloat16)
    mean_part = xbar + jnp.sum(gain.astype(jnp.float32) * wvec, axis=-1)
    update = jnp.dot(gain.reshape(-1, n_obs), zmat, preferred_element_type=jnp.float32)
    anom_part = (flat.astype(jnp.float32) - update).astype(jnp.bfloat16).reshape(block.shape)
    return (mean_part, anom_part)


def local(state, obs_col, obs_row, foot_off, obs_lev, obs_val, obs_err, loc):
    level_groups = lax.axis_size("lev")
    ny_total = loc.shape[1] * lax.axis_size("gy") * level_groups
    x_count, y_count, lev_count, members = state.shape
    code = footprint_code(
        obs_col, obs_row, foot_off, obs_lev, (y_count, lev_count), ny_total,
        lax.axis_index("gy") * y_count, lax.axis_index("lev") * lev_count,
    )
    zmat, wcol, ybf, relaid = analysis_weights(state, code, obs_val, obs_err)
    block = relaid.transpose(1, 2, 0, 3, 4).reshape(x_count, loc.shape[1], -1, members)
    return analyse(block, loc, zmat, wcol[:, 0], ybf)


def solution(mesh):
    return jax.shard_map(
        local,
        mesh=mesh,
        in_specs=(
            P("gx", "gy", "lev", None),
            P("gx"),
            P("gx"),
            P("gx", None),
            P("gx"),
            P("gx"),
            P("gx"),
            P("gx", ("gy", "lev"), None),
        ),
        out_specs=(P("gx", ("gy", "lev"), None), P("gx", ("gy", "lev"), None, None)),
        check_vma=False,
    )
```

```python
import functools

import jax
import jax.numpy as jnp
from jax import lax
from jax.experimental import pallas as pl
from jax.experimental.pallas import tpu as pltpu
from jax.sharding import PartitionSpec as P

KF = 8
HW = 8
DY = 2
SUB = 8
LANES = 128
BLOCK = 64
MESH = pl.DeviceIdType.MESH


def footprint_code(obs_col, obs_row, foot_off, obs_lev, shape, ny_total, y_start, lev_start):
    x_count, y_count, lev_count = shape
    planes = y_count * lev_count
    span = 2 * DY + 1
    shift_x = foot_off // span - HW
    shift_y = foot_off % span - DY
    x_here = obs_col[:, None] + shift_x
    y_here = jnp.clip(obs_row[:, None] + shift_y, 0, ny_total - 1) - y_start
    lev_here = obs_lev[:, None] - lev_start
    inside = (y_here >= 0) & (y_here < y_count) & (lev_here >= 0) & (lev_here < lev_count)
    plane = y_here * lev_count + lev_here
    middle = plane * x_count + x_here
    before = planes * x_count + plane * HW + x_here + HW
    after = planes * (x_count + HW) + plane * HW + x_here - x_count
    spot = jnp.where(x_here < 0, before, jnp.where(x_here < x_count, middle, after))
    return jnp.where(inside, spot, -1)


def lane_cast(value, k):
    return jnp.broadcast_to(value[:, k : k + 1], value.shape)


def row_cast(value, i):
    return jnp.broadcast_to(value[i : i + 1, :], value.shape)


def f32_dot(a, b, dims):
    return lax.dot_general(
        a, b, (dims, ((), ())), precision=lax.Precision.HIGHEST, preferred_element_type=jnp.float32
    )


def factor_block(w_ref, x_ref, root_err):
    rows = w_ref.shape[0]
    groups = rows // SUB
    w = [w_ref[SUB * g : SUB * (g + 1), :] for g in range(groups)]
    x = [x_ref[SUB * g : SUB * (g + 1), :] for g in range(groups)]
    sub_id = lax.broadcasted_iota(jnp.int32, (SUB, LANES), 0)
    for g in range(groups):
        col = {h: [lane_cast(w[h], SUB * g + m) for m in range(SUB)] for h in range(g, groups)}
        s = {(i, m): row_cast(col[g][m], i) for m in range(SUB) for i in range(m, SUB)}
        wr = [row_cast(w[g], i) for i in range(SUB)]
        xr = [row_cast(x[g], i) for i in range(SUB)]
        inv = []
        for k in range(SUB):
            pivot = s[k, k]
            inv_k = lax.rsqrt(pivot)
            inv.append(inv_k)
            minv_k = 1.0 / (pivot * inv_k + row_cast(root_err[g], k))
            for i in range(k + 1, SUB):
                s[i, k] = s[i, k] * inv_k
            for m in range(k + 1, SUB):
                for i in range(m, SUB):
                    s[i, m] = s[i, m] - s[i, k] * s[m, k]
            wr[k] = wr[k] * inv_k
            xr[k] = xr[k] * minv_k
            for i in range(k + 1, SUB):
                wr[i] = wr[i] - s[i, k] * wr[k]
                xr[i] = xr[i] - s[i, k] * xr[k]
        w_new, x_new = wr[0], xr[0]
        for k in range(1, SUB):
            w_new = jnp.where(sub_id == k, wr[k], w_new)
            x_new = jnp.where(sub_id == k, xr[k], x_new)
        w[g], x[g] = w_new, x_new
        for k in reversed(range(SUB)):
            wr[k] = wr[k] * inv[k]
            xr[k] = xr[k] * inv[k]
            for i in range(k):
                wr[i] = wr[i] - s[k, i] * wr[k]
                xr[i] = xr[i] - s[k, i] * xr[k]
        for h in range(g + 1, groups):
            for m in range(SUB):
                w[h] = w[h] - col[h][m] * wr[m]
                x[h] = x[h] - col[h][m] * xr[m]
    for g in range(groups):
        w_ref[SUB * g : SUB * (g + 1), :] = w[g]
        x_ref[SUB * g : SUB * (g + 1), :] = x[g]


def solve_weights(err_ref, z_ref, w_out_ref, y_ref, a_ref, s_ref, root_ref, w_ref, x_ref, inv_ref, low_ref):
    n, members = y_ref.shape
    blocks = n // BLOCK
    ybf = s_ref[:, :members].astype(jnp.bfloat16)
    y_ref[...] = ybf
    root_ref[...] = jnp.broadcast_to(jnp.sqrt(err_ref[...]), (n, LANES))
    same = lax.broadcasted_iota(jnp.int32, (n, n), 0) == lax.broadcasted_iota(jnp.int32, (n, n), 1)
    a_ref[...] = lax.dot_general(ybf, ybf, (((1,), (1,)), ((), ())), preferred_element_type=jnp.float32) / (members - 1) + jnp.where(same, err_ref[...], 0.0)
    eye_w = lax.broadcasted_iota(jnp.int32, (BLOCK, LANES), 0) + BLOCK == lax.broadcasted_iota(jnp.int32, (BLOCK, LANES), 1)
    eye_x = lax.broadcasted_iota(jnp.int32, (BLOCK, LANES), 0) == lax.broadcasted_iota(jnp.int32, (BLOCK, LANES), 1)

    def load_block(at):
        w_ref[...] = jnp.where(eye_w, 1.0, 0.0)
        w_ref[:, :BLOCK] = a_ref[at : at + BLOCK, at : at + BLOCK]
        x_ref[...] = jnp.where(eye_x, 1.0, 0.0)

    load_block(0)

    def step(k, carry):
        base = pl.multiple_of(k * BLOCK, BLOCK)
        root_err = [root_ref[pl.ds(base + SUB * g, SUB), :] for g in range(BLOCK // SUB)]
        factor_block(w_ref, x_ref, root_err)
        for kk in range(blocks):

            @pl.when(k == kk)
            def _():
                at, end = kk * BLOCK, (kk + 1) * BLOCK
                l_inv = w_ref[:, BLOCK:]
                m_inv = x_ref[:, :BLOCK]
                inv_ref[kk] = l_inv
                s_ref[at:end, :members] = f32_dot(m_inv, s_ref[at:end, :members], ((1,), (0,)))
                s_ref[at:end, members:] = f32_dot(l_inv, s_ref[at:end, members:], ((1,), (0,)))
                if end < n:
                    left = end // LANES * LANES
                    panel = f32_dot(a_ref[left:, at:end], l_inv, ((1,), (1,)))
                    below = panel[end - left :]
                    low_ref[kk, end:, :] = below
                    a_ref[end:, left:] = a_ref[end:, left:] - f32_dot(below, panel, ((1,), (1,)))
                    load_block(end)
                    s_ref[end:, :] = s_ref[end:, :] - f32_dot(below, s_ref[at:end, :], ((1,), (0,)))

        return carry

    lax.fori_loop(0, blocks, step, 0)
    for kk in reversed(range(blocks)):
        at, end = kk * BLOCK, (kk + 1) * BLOCK
        right = s_ref[at:end, :]
        if end < n:
            right = right - f32_dot(low_ref[kk, end:, :], s_ref[end:, :], ((0,), (0,)))
        s_ref[at:end, :] = f32_dot(inv_ref[kk], right, ((0,), (0,)))
    z_ref[...] = s_ref[:, :members].astype(jnp.bfloat16)
    w_out_ref[...] = s_ref[:, members:]


def analysis_weights_kernel(
    axes, code_ref, state_ref, val_ref, err_ref, z_ref, w_out_ref, y_ref, relaid_ref,
    acc_ref, before_ref, after_ref, zin_ref, ys_ref, hb_ref, half_refs,
    a_ref, s_ref, root_ref, w_ref, x_ref, inv_ref, low_ref, send_sem, recv_sem, own_sem,
):
    gxs, gys, levs = axes
    gx, gy, lev = lax.axis_index("gx"), lax.axis_index("gy"), lax.axis_index("lev")
    n, members = acc_ref.shape
    planes, x_count = state_ref.shape[:2]
    edge, inner = planes * HW, planes * x_count
    share = planes // levs
    right, left = lax.rem(gx + 1, gxs), lax.rem(gx + gxs - 1, gxs)
    levels = [(lax.rem(lev + d, levs)) for d in range(1, levs)]
    lats = [(lax.rem(gy + d, gys)) for d in range(1, gys)]
    barrier = pltpu.get_barrier_semaphore()
    peers = [{"gx": right}, {"gx": left}] + [{"lev": v} for v in levels] + [{"gy": v} for v in lats]
    for peer in peers:
        pl.semaphore_signal(barrier, inc=1, device_id=peer, device_id_type=MESH)
    pl.semaphore_wait(barrier, len(peers))
    count = [0]

    def remote(src, dst, peer):
        i = count[0]
        count[0] += 1
        return pltpu.make_async_remote_copy(
            src_ref=src, dst_ref=dst, send_sem=send_sem.at[i], recv_sem=recv_sem.at[i],
            device_id=peer, device_id_type=MESH,
        )

    halo = [
        remote(state_ref.at[:, x_count - HW :], before_ref, {"gx": right}),
        remote(state_ref.at[:, :HW], after_ref, {"gx": left}),
    ]
    for copy in halo:
        copy.start()
    own = pltpu.make_async_copy(state_ref.at[pl.ds(lev * share, share)], relaid_ref.at[lev], own_sem.at[0])
    own.start()

    def chosen(base, width):
        spot = lax.broadcasted_iota(jnp.int32, (n, width), 1) + base
        hits = jnp.zeros((n, width), jnp.float32)
        for slot in range(KF):
            hits = hits + jnp.where(code_ref[:, slot : slot + 1] == spot, 1.0, 0.0)
        return hits.astype(jnp.bfloat16)

    def flat(ref):
        return ref[...].astype(jnp.float32).reshape(edge, members).astype(jnp.bfloat16)

    acc_ref[...] = jnp.zeros_like(acc_ref)

    def pick(i, carry):
        acc_ref[...] += jnp.dot(
            chosen(i * x_count, x_count), state_ref[i], preferred_element_type=jnp.float32
        )
        return carry

    lax.fori_loop(0, planes, pick, 0)
    sel_before, sel_after = chosen(inner, edge), chosen(inner + edge, edge)
    for copy in halo:
        copy.wait()
    acc_ref[...] += jnp.dot(sel_before, flat(before_ref), preferred_element_type=jnp.float32) + jnp.dot(
        sel_after, flat(after_ref), preferred_element_type=jnp.float32
    )
    base, size = 0, n
    bits = levs.bit_length() - 1
    bases = []
    for b in range(bits):
        size //= 2
        bit = lax.rem(lev // (1 << b), 2)
        partner = lev + (1 - 2 * bit) * (1 << b)
        keep, give = base + bit * size, base + (1 - bit) * size
        copy = remote(acc_ref.at[pl.ds(pl.multiple_of(give, 8), size)], half_refs[b], {"lev": partner})
        copy.start()
        copy.wait()
        rows = pl.ds(pl.multiple_of(keep, 8), size)
        acc_ref[rows, :] = acc_ref[rows, :] + half_refs[b][...]
        base = keep
        bases.append((base, size, partner))
    part = n // (levs * gys)
    copies = []
    for d, lat in enumerate(lats):
        copies.append(
            remote(acc_ref.at[pl.ds(pl.multiple_of(base + lat * part, 8), part)], zin_ref.at[d], {"gy": lat})
        )
    for copy in copies:
        copy.start()
    for copy in copies:
        copy.wait()
    mine = base + gy * part
    total = acc_ref[pl.ds(pl.multiple_of(mine, 8), part), :]
    for d in range(gys - 1):
        total = total + zin_ref[d]
    hx = total / KF
    hbar = jnp.mean(hx, axis=1, keepdims=True)
    chunk = base // part + gy
    ys_ref[chunk] = (hx - hbar).astype(jnp.bfloat16)
    hb_ref[chunk] = jnp.broadcast_to(hbar, (part, LANES))
    copies = []
    for lat in lats:
        copies.append(remote(ys_ref.at[chunk], ys_ref.at[chunk], {"gy": lat}))
        copies.append(remote(hb_ref.at[chunk], hb_ref.at[chunk], {"gy": lat}))
    for copy in copies:
        copy.start()
    for copy in copies:
        copy.wait()
    for start, size, partner in reversed(bases):
        span = pl.ds(start // part, size // part)
        copies = [
            remote(ys_ref.at[span], ys_ref.at[span], {"lev": partner}),
            remote(hb_ref.at[span], hb_ref.at[span], {"lev": partner}),
        ]
        for copy in copies:
            copy.start()
        for copy in copies:
            copy.wait()
    copies = [
        remote(state_ref.at[pl.ds(v * share, share)], relaid_ref.at[lev], {"lev": v}) for v in levels
    ]
    for copy in copies:
        copy.start()
    for c in range(levs * gys):
        s_ref[c * part : (c + 1) * part, :members] = ys_ref[c].astype(jnp.float32)
        s_ref[c * part : (c + 1) * part, members:] = val_ref[c * part : (c + 1) * part, :] - hb_ref[c]
    solve_weights(err_ref, z_ref, w_out_ref, y_ref, a_ref, s_ref, root_ref, w_ref, x_ref, inv_ref, low_ref)
    for copy in copies:
        copy.wait()
    own.wait()


def analysis_weights(state, code, values, errors):
    axes = tuple(lax.axis_size(name) for name in ("gx", "gy", "lev"))
    gxs, gys, levs = axes
    planes, x_count, members = state.shape
    n = values.shape[0]
    part = n // (gys * levs)
    bits = levs.bit_length() - 1
    copies = 2 + bits + (gys - 1) + 2 * (gys - 1) + 2 * bits + (levs - 1)
    vmem = pl.BlockSpec(memory_space=pltpu.VMEM)
    hbm = pl.BlockSpec(memory_space=pl.ANY)
    return pl.pallas_call(
        functools.partial(analysis_weights_kernel, axes),
        name="analysis_weights",
        out_shape=(
            jax.ShapeDtypeStruct((n, members), jnp.bfloat16),
            jax.ShapeDtypeStruct((n, LANES), jnp.float32),
            jax.ShapeDtypeStruct((n, members), jnp.bfloat16),
            jax.ShapeDtypeStruct((levs, planes // levs, x_count, members), jnp.bfloat16),
        ),
        in_specs=[vmem, vmem, vmem, vmem],
        out_specs=(vmem, vmem, vmem, hbm),
        scratch_shapes=[
            pltpu.VMEM((n, members), jnp.float32),
            pltpu.VMEM((planes, HW, members), jnp.bfloat16),
            pltpu.VMEM((planes, HW, members), jnp.bfloat16),
            pltpu.VMEM((gys - 1, part, members), jnp.float32),
            pltpu.VMEM((gys * levs, part, members), jnp.bfloat16),
            pltpu.VMEM((gys * levs, part, LANES), jnp.float32),
            [pltpu.VMEM((n >> (b + 1), members), jnp.float32) for b in range(bits)],
            pltpu.VMEM((n, n), jnp.float32),
            pltpu.VMEM((n, members + LANES), jnp.float32),
            pltpu.VMEM((n, LANES), jnp.float32),
            pltpu.VMEM((BLOCK, LANES), jnp.float32),
            pltpu.VMEM((BLOCK, LANES), jnp.float32),
            pltpu.VMEM((n // BLOCK, BLOCK, BLOCK), jnp.float32),
            pltpu.VMEM((n // BLOCK, n, BLOCK), jnp.float32),
            pltpu.SemaphoreType.DMA((copies,)),
            pltpu.SemaphoreType.DMA((copies,)),
            pltpu.SemaphoreType.DMA((1,)),
        ],
        compiler_params=pltpu.CompilerParams(
            collective_id=0, has_side_effects=True, vmem_limit_bytes=48 * 1024 * 1024
        ),
    )(code, state, values[:, None], errors[:, None])


def analyse_kernel(relaid_ref, loc_ref, z_ref, y_ref, w_ref, mean_ref, out_ref, rows_ref):
    levs, share, width, members = relaid_ref.shape
    lats = loc_ref.shape[0]
    pairs = share // lats
    stride = lats * levs * pairs
    block = relaid_ref[...].reshape(levs * share * width, members).astype(jnp.float32)
    xbar = jnp.mean(block, axis=1, keepdims=True)
    anom = (block - xbar).astype(jnp.bfloat16)
    cross = lax.dot_general(
        anom, y_ref[...], (((1,), (1,)), ((), ())), preferred_element_type=jnp.float32
    ) * (1.0 / (members - 1))
    parts = []
    for lev in range(levs):
        for lat in range(lats):
            weight = loc_ref[lat].astype(jnp.float32)
            for pair in range(pairs):
                at = (lev * share + lat * pairs + pair) * width
                parts.append((cross[at : at + width] * weight).astype(jnp.bfloat16))
    gain = jnp.concatenate(parts, axis=0)
    mean = xbar + jnp.sum(gain.astype(jnp.float32) * w_ref[...], axis=1, keepdims=True)
    update = jnp.dot(gain, z_ref[...], preferred_element_type=jnp.float32)
    result = anom.astype(jnp.float32) - update
    lane = lax.broadcasted_iota(jnp.int32, (width, LANES), 1)
    means = jnp.zeros((width, LANES), jnp.float32)
    for lev in range(levs):
        for lat in range(lats):
            for pair in range(pairs):
                at = (lev * share + lat * pairs + pair) * width
                spot = lat * levs * pairs + lev * pairs + pair
                means = jnp.where(lane == spot, jnp.broadcast_to(mean[at : at + width], (width, LANES)), means)
                for c in range(members // LANES):
                    rows_ref[c, pl.ds(spot, width, stride=stride), :] = result[
                        at : at + width, c * LANES : (c + 1) * LANES
                    ]
    mean_ref[...] = means
    for c in range(members // LANES):
        out_ref[:, c * LANES : (c + 1) * LANES] = rows_ref[c].astype(jnp.bfloat16)


def analyse(relaid, loc, zmat, wvec, ybf):
    levs, share, x_count, members = relaid.shape
    lats, n = loc.shape[1], ybf.shape[0]
    planes = levs * share
    width = min(32, x_count)
    means, out = pl.pallas_call(
        analyse_kernel,
        name="analyse",
        grid=(x_count // width,),
        out_shape=(
            jax.ShapeDtypeStruct((x_count, LANES), jnp.float32),
            jax.ShapeDtypeStruct((x_count * planes, members), jnp.bfloat16),
        ),
        in_specs=[
            pl.BlockSpec((levs, share, width, members), lambda i: (0, 0, i, 0)),
            pl.BlockSpec((lats, width, n), lambda i: (0, i, 0)),
            pl.BlockSpec((n, members), lambda i: (0, 0)),
            pl.BlockSpec((n, members), lambda i: (0, 0)),
            pl.BlockSpec((1, n), lambda i: (0, 0)),
        ],
        out_specs=(
            pl.BlockSpec((width, LANES), lambda i: (i, 0)),
            pl.BlockSpec((width * planes, members), lambda i: (i, 0)),
        ),
        scratch_shapes=[pltpu.VMEM((members // LANES, width * planes, LANES), jnp.float32)],
        compiler_params=pltpu.CompilerParams(vmem_limit_bytes=48 * 1024 * 1024),
    )(relaid, loc.transpose(1, 0, 2), zmat, ybf, wvec[None, :])
    per_lat = planes // lats
    return (
        means[:, :planes].reshape(x_count, lats, per_lat),
        out.reshape(x_count, lats, per_lat, members),
    )


def local(state, obs_col, obs_row, foot_off, obs_lev, obs_val, obs_err, loc):
    level_groups = lax.axis_size("lev")
    ny_total = loc.shape[1] * lax.axis_size("gy") * level_groups
    x_count, y_count, lev_count, members = state.shape
    code = footprint_code(
        obs_col, obs_row, foot_off, obs_lev, (x_count, y_count, lev_count), ny_total,
        lax.axis_index("gy") * y_count, lax.axis_index("lev") * lev_count,
    )
    planes = state.transpose(1, 2, 0, 3).reshape(y_count * lev_count, x_count, members)
    zmat, wcol, ybf, relaid = analysis_weights(planes, code, obs_val, obs_err)
    return analyse(relaid, loc, zmat, wcol[:, 0], ybf)


def solution(mesh):
    return jax.shard_map(
        local,
        mesh=mesh,
        in_specs=(
            P("gx", "gy", "lev", None),
            P("gx"),
            P("gx"),
            P("gx", None),
            P("gx"),
            P("gx"),
            P("gx"),
            P("gx", ("gy", "lev"), None),
        ),
        out_specs=(P("gx", ("gy", "lev"), None), P("gx", ("gy", "lev"), None, None)),
        check_vma=False,
    )
```

```python
import functools

import jax
import jax.numpy as jnp
from jax import lax
from jax.experimental import pallas as pl
from jax.experimental.pallas import tpu as pltpu
from jax.sharding import PartitionSpec as P

KF = 8
HW = 8
DY = 2
SUB = 8
LANES = 128
BLOCK = 64
MESH = pl.DeviceIdType.MESH


def footprint_code(obs_col, obs_row, foot_off, obs_lev, shape, ny_total, y_start, lev_start):
    x_count, y_count, lev_count = shape
    planes = y_count * lev_count
    span = 2 * DY + 1
    shift_x = foot_off // span - HW
    shift_y = foot_off % span - DY
    x_here = obs_col[:, None] + shift_x
    y_here = jnp.clip(obs_row[:, None] + shift_y, 0, ny_total - 1) - y_start
    lev_here = obs_lev[:, None] - lev_start
    inside = (y_here >= 0) & (y_here < y_count) & (lev_here >= 0) & (lev_here < lev_count)
    plane = y_here * lev_count + lev_here
    middle = plane * x_count + x_here
    before = planes * x_count + plane * HW + x_here + HW
    after = planes * (x_count + HW) + plane * HW + x_here - x_count
    spot = jnp.where(x_here < 0, before, jnp.where(x_here < x_count, middle, after))
    return jnp.where(inside, spot, -1)


def lane_cast(value, k):
    return jnp.broadcast_to(value[:, k : k + 1], value.shape)


def row_cast(value, i):
    return jnp.broadcast_to(value[i : i + 1, :], value.shape)


def f32_dot(a, b, dims):
    return lax.dot_general(
        a, b, (dims, ((), ())), precision=lax.Precision.HIGHEST, preferred_element_type=jnp.float32
    )


def split_dot(a, b, dims):
    a_high, b_high = a.astype(jnp.bfloat16), b.astype(jnp.bfloat16)
    a_low = (a - a_high.astype(jnp.float32)).astype(jnp.bfloat16)
    b_low = (b - b_high.astype(jnp.float32)).astype(jnp.bfloat16)

    def dot(left, right):
        return lax.dot_general(left, right, (dims, ((), ())), preferred_element_type=jnp.float32)

    return dot(a_high, b_high) + (dot(a_high, b_low) + dot(a_low, b_high))


def factor_block(w_ref, x_ref, root_err):
    rows = w_ref.shape[0]
    groups = rows // SUB
    w = [w_ref[SUB * g : SUB * (g + 1), :] for g in range(groups)]
    x = [x_ref[SUB * g : SUB * (g + 1), :] for g in range(groups)]
    sub_id = lax.broadcasted_iota(jnp.int32, (SUB, LANES), 0)
    for g in range(groups):
        col = {h: [lane_cast(w[h], SUB * g + m) for m in range(SUB)] for h in range(g, groups)}
        s = {(i, m): row_cast(col[g][m], i) for m in range(SUB) for i in range(m, SUB)}
        wr = [row_cast(w[g], i) for i in range(SUB)]
        xr = [row_cast(x[g], i) for i in range(SUB)]
        inv = []
        for k in range(SUB):
            pivot = s[k, k]
            inv_k = lax.rsqrt(pivot)
            inv.append(inv_k)
            minv_k = 1.0 / (pivot * inv_k + row_cast(root_err[g], k))
            for i in range(k + 1, SUB):
                s[i, k] = s[i, k] * inv_k
            for m in range(k + 1, SUB):
                for i in range(m, SUB):
                    s[i, m] = s[i, m] - s[i, k] * s[m, k]
            wr[k] = wr[k] * inv_k
            xr[k] = xr[k] * minv_k
            for i in range(k + 1, SUB):
                wr[i] = wr[i] - s[i, k] * wr[k]
                xr[i] = xr[i] - s[i, k] * xr[k]
        w_new, x_new = wr[0], xr[0]
        for k in range(1, SUB):
            w_new = jnp.where(sub_id == k, wr[k], w_new)
            x_new = jnp.where(sub_id == k, xr[k], x_new)
        w[g], x[g] = w_new, x_new
        for k in reversed(range(SUB)):
            wr[k] = wr[k] * inv[k]
            xr[k] = xr[k] * inv[k]
            for i in range(k):
                wr[i] = wr[i] - s[k, i] * wr[k]
                xr[i] = xr[i] - s[k, i] * xr[k]
        for h in range(g + 1, groups):
            for m in range(SUB):
                w[h] = w[h] - col[h][m] * wr[m]
                x[h] = x[h] - col[h][m] * xr[m]
    for g in range(groups):
        w_ref[SUB * g : SUB * (g + 1), :] = w[g]
        x_ref[SUB * g : SUB * (g + 1), :] = x[g]


def solve_weights(err_ref, z_ref, w_out_ref, y_ref, a_ref, s_ref, root_ref, w_ref, x_ref, inv_ref, low_ref):
    n, members = y_ref.shape
    blocks = n // BLOCK
    ybf = s_ref[:, :members].astype(jnp.bfloat16)
    y_ref[...] = ybf
    root_ref[...] = jnp.broadcast_to(jnp.sqrt(err_ref[...]), (n, LANES))
    same = lax.broadcasted_iota(jnp.int32, (n, n), 0) == lax.broadcasted_iota(jnp.int32, (n, n), 1)
    a_ref[...] = lax.dot_general(ybf, ybf, (((1,), (1,)), ((), ())), preferred_element_type=jnp.float32) / (members - 1) + jnp.where(same, err_ref[...], 0.0)
    eye_w = lax.broadcasted_iota(jnp.int32, (BLOCK, LANES), 0) + BLOCK == lax.broadcasted_iota(jnp.int32, (BLOCK, LANES), 1)
    eye_x = lax.broadcasted_iota(jnp.int32, (BLOCK, LANES), 0) == lax.broadcasted_iota(jnp.int32, (BLOCK, LANES), 1)

    def load_block(at):
        w_ref[...] = jnp.where(eye_w, 1.0, 0.0)
        w_ref[:, :BLOCK] = a_ref[at : at + BLOCK, at : at + BLOCK]
        x_ref[...] = jnp.where(eye_x, 1.0, 0.0)

    load_block(0)

    def step(k, carry):
        base = pl.multiple_of(k * BLOCK, BLOCK)
        root_err = [root_ref[pl.ds(base + SUB * g, SUB), :] for g in range(BLOCK // SUB)]
        factor_block(w_ref, x_ref, root_err)
        for kk in range(blocks):

            @pl.when(k == kk)
            def _():
                at, end = kk * BLOCK, (kk + 1) * BLOCK
                l_inv = w_ref[:, BLOCK:]
                m_inv = x_ref[:, :BLOCK]
                inv_ref[kk] = l_inv
                s_ref[at:end, :members] = f32_dot(m_inv, s_ref[at:end, :members], ((1,), (0,)))
                s_ref[at:end, members:] = f32_dot(l_inv, s_ref[at:end, members:], ((1,), (0,)))
                if end < n:
                    left = end // LANES * LANES
                    panel = f32_dot(a_ref[left:, at:end], l_inv, ((1,), (1,)))
                    below = panel[end - left :]
                    low_ref[kk, end:, :] = below
                    a_ref[end:, left:] = a_ref[end:, left:] - f32_dot(below, panel, ((1,), (1,)))
                    load_block(end)
                    s_ref[end:, :] = s_ref[end:, :] - split_dot(below, s_ref[at:end, :], ((1,), (0,)))

        return carry

    lax.fori_loop(0, blocks, step, 0)
    for kk in reversed(range(blocks)):
        at, end = kk * BLOCK, (kk + 1) * BLOCK
        right = s_ref[at:end, :]
        if end < n:
            right = right - split_dot(low_ref[kk, end:, :], s_ref[end:, :], ((0,), (0,)))
        s_ref[at:end, :] = f32_dot(inv_ref[kk], right, ((0,), (0,)))
    z_ref[...] = s_ref[:, :members].astype(jnp.bfloat16)
    w_out_ref[...] = s_ref[:, members:]


def analysis_weights_kernel(
    axes, code_ref, state_ref, val_ref, err_ref, z_ref, w_out_ref, y_ref, relaid_ref,
    acc_ref, before_ref, after_ref, zin_ref, ys_ref, hb_ref, half_refs,
    a_ref, s_ref, root_ref, w_ref, x_ref, inv_ref, low_ref, send_sem, recv_sem, own_sem,
):
    gxs, gys, levs = axes
    gx, gy, lev = lax.axis_index("gx"), lax.axis_index("gy"), lax.axis_index("lev")
    n, members = acc_ref.shape
    planes, x_count = state_ref.shape[:2]
    edge, inner = planes * HW, planes * x_count
    share = planes // levs
    right, left = lax.rem(gx + 1, gxs), lax.rem(gx + gxs - 1, gxs)
    levels = [(lax.rem(lev + d, levs)) for d in range(1, levs)]
    lats = [(lax.rem(gy + d, gys)) for d in range(1, gys)]
    barrier = pltpu.get_barrier_semaphore()
    peers = [{"gx": right}, {"gx": left}] + [{"lev": v} for v in levels] + [{"gy": v} for v in lats]
    for peer in peers:
        pl.semaphore_signal(barrier, inc=1, device_id=peer, device_id_type=MESH)
    pl.semaphore_wait(barrier, len(peers))
    count = [0]

    def remote(src, dst, peer):
        i = count[0]
        count[0] += 1
        return pltpu.make_async_remote_copy(
            src_ref=src, dst_ref=dst, send_sem=send_sem.at[i], recv_sem=recv_sem.at[i],
            device_id=peer, device_id_type=MESH,
        )

    halo = [
        remote(state_ref.at[:, x_count - HW :], before_ref, {"gx": right}),
        remote(state_ref.at[:, :HW], after_ref, {"gx": left}),
    ]
    for copy in halo:
        copy.start()
    own = pltpu.make_async_copy(state_ref.at[pl.ds(lev * share, share)], relaid_ref.at[lev], own_sem.at[0])
    own.start()

    def chosen(base, width):
        spot = lax.broadcasted_iota(jnp.int32, (n, width), 1) + base
        hits = jnp.zeros((n, width), jnp.float32)
        for slot in range(KF):
            hits = hits + jnp.where(code_ref[:, slot : slot + 1] == spot, 1.0, 0.0)
        return hits.astype(jnp.bfloat16)

    def flat(ref):
        return ref[...].astype(jnp.float32).reshape(edge, members).astype(jnp.bfloat16)

    acc_ref[...] = jnp.zeros_like(acc_ref)

    batch = 4 if planes % 4 == 0 else 1

    def pick(i, carry):
        rows = state_ref[pl.ds(i * batch, batch)].reshape(batch * x_count, members)
        acc_ref[...] += jnp.dot(
            chosen(i * (batch * x_count), batch * x_count), rows, preferred_element_type=jnp.float32
        )
        return carry

    lax.fori_loop(0, planes // batch, pick, 0)
    sel_before, sel_after = chosen(inner, edge), chosen(inner + edge, edge)
    for copy in halo:
        copy.wait()
    acc_ref[...] += jnp.dot(sel_before, flat(before_ref), preferred_element_type=jnp.float32) + jnp.dot(
        sel_after, flat(after_ref), preferred_element_type=jnp.float32
    )
    base, size = 0, n
    bits = levs.bit_length() - 1
    bases = []
    for b in range(bits):
        size //= 2
        bit = lax.rem(lev // (1 << b), 2)
        partner = lev + (1 - 2 * bit) * (1 << b)
        keep, give = base + bit * size, base + (1 - bit) * size
        copy = remote(acc_ref.at[pl.ds(pl.multiple_of(give, 8), size)], half_refs[b], {"lev": partner})
        copy.start()
        copy.wait()
        rows = pl.ds(pl.multiple_of(keep, 8), size)
        acc_ref[rows, :] = acc_ref[rows, :] + half_refs[b][...]
        base = keep
        bases.append((base, size, partner))
    part = n // (levs * gys)
    copies = []
    for d, lat in enumerate(lats):
        copies.append(
            remote(acc_ref.at[pl.ds(pl.multiple_of(base + lat * part, 8), part)], zin_ref.at[d], {"gy": lat})
        )
    for copy in copies:
        copy.start()
    for copy in copies:
        copy.wait()
    mine = base + gy * part
    total = acc_ref[pl.ds(pl.multiple_of(mine, 8), part), :]
    for d in range(gys - 1):
        total = total + zin_ref[d]
    hx = total / KF
    hbar = jnp.mean(hx, axis=1, keepdims=True)
    chunk = base // part + gy
    ys_ref[chunk] = (hx - hbar).astype(jnp.bfloat16)
    diagonal = lax.broadcasted_iota(jnp.int32, (part, LANES), 0) == lax.broadcasted_iota(
        jnp.int32, (part, LANES), 1
    )
    row = jnp.sum(jnp.where(diagonal, hbar, 0.0), axis=0, keepdims=True)
    hb_ref[chunk] = jnp.broadcast_to(row, (SUB, LANES))
    copies = []
    for lat in lats:
        copies.append(remote(ys_ref.at[chunk], ys_ref.at[chunk], {"gy": lat}))
        copies.append(remote(hb_ref.at[chunk], hb_ref.at[chunk], {"gy": lat}))
    for copy in copies:
        copy.start()
    for copy in copies:
        copy.wait()
    for start, size, partner in reversed(bases):
        span = pl.ds(start // part, size // part)
        copies = [
            remote(ys_ref.at[span], ys_ref.at[span], {"lev": partner}),
            remote(hb_ref.at[span], hb_ref.at[span], {"lev": partner}),
        ]
        for copy in copies:
            copy.start()
        for copy in copies:
            copy.wait()
    copies = [
        remote(state_ref.at[pl.ds(v * share, share)], relaid_ref.at[lev], {"lev": v}) for v in levels
    ]
    for copy in copies:
        copy.start()
    for c in range(levs * gys):
        s_ref[c * part : (c + 1) * part, :members] = ys_ref[c].astype(jnp.float32)
        center = jnp.sum(
            jnp.where(diagonal, jnp.broadcast_to(hb_ref[c][:1, :], (part, LANES)), 0.0), axis=1, keepdims=True
        )
        s_ref[c * part : (c + 1) * part, members:] = jnp.broadcast_to(
            val_ref[c * part : (c + 1) * part, :] - center, (part, LANES)
        )
    solve_weights(err_ref, z_ref, w_out_ref, y_ref, a_ref, s_ref, root_ref, w_ref, x_ref, inv_ref, low_ref)
    for copy in copies:
        copy.wait()
    own.wait()


def analysis_weights(state, code, values, errors):
    axes = tuple(lax.axis_size(name) for name in ("gx", "gy", "lev"))
    gxs, gys, levs = axes
    planes, x_count, members = state.shape
    n = values.shape[0]
    part = n // (gys * levs)
    bits = levs.bit_length() - 1
    copies = 2 + bits + (gys - 1) + 2 * (gys - 1) + 2 * bits + (levs - 1)
    vmem = pl.BlockSpec(memory_space=pltpu.VMEM)
    hbm = pl.BlockSpec(memory_space=pl.ANY)
    return pl.pallas_call(
        functools.partial(analysis_weights_kernel, axes),
        name="analysis_weights",
        out_shape=(
            jax.ShapeDtypeStruct((n, members), jnp.bfloat16),
            jax.ShapeDtypeStruct((n, LANES), jnp.float32),
            jax.ShapeDtypeStruct((n, members), jnp.bfloat16),
            jax.ShapeDtypeStruct((levs, planes // levs, x_count, members), jnp.bfloat16),
        ),
        in_specs=[vmem, vmem, vmem, vmem],
        out_specs=(vmem, vmem, vmem, hbm),
        scratch_shapes=[
            pltpu.VMEM((n, members), jnp.float32),
            pltpu.VMEM((planes, HW, members), jnp.bfloat16),
            pltpu.VMEM((planes, HW, members), jnp.bfloat16),
            pltpu.VMEM((gys - 1, part, members), jnp.float32),
            pltpu.VMEM((gys * levs, part, members), jnp.bfloat16),
            pltpu.VMEM((gys * levs, SUB, LANES), jnp.float32),
            [pltpu.VMEM((n >> (b + 1), members), jnp.float32) for b in range(bits)],
            pltpu.VMEM((n, n), jnp.float32),
            pltpu.VMEM((n, members + LANES), jnp.float32),
            pltpu.VMEM((n, LANES), jnp.float32),
            pltpu.VMEM((BLOCK, LANES), jnp.float32),
            pltpu.VMEM((BLOCK, LANES), jnp.float32),
            pltpu.VMEM((n // BLOCK, BLOCK, BLOCK), jnp.float32),
            pltpu.VMEM((n // BLOCK, n, BLOCK), jnp.float32),
            pltpu.SemaphoreType.DMA((copies,)),
            pltpu.SemaphoreType.DMA((copies,)),
            pltpu.SemaphoreType.DMA((1,)),
        ],
        compiler_params=pltpu.CompilerParams(
            collective_id=0, has_side_effects=True, vmem_limit_bytes=48 * 1024 * 1024
        ),
    )(code, state, values[:, None], errors[:, None])


def analyse_kernel(relaid_ref, loc_ref, z_ref, y_ref, w_ref, mean_ref, out_ref, rows_ref):
    levs, share, width, members = relaid_ref.shape
    lats = loc_ref.shape[0]
    pairs = share // lats
    stride = lats * levs * pairs
    block = relaid_ref[...].reshape(levs * share * width, members).astype(jnp.float32)
    xbar = jnp.mean(block, axis=1, keepdims=True)
    anom = (block - xbar).astype(jnp.bfloat16)
    cross = lax.dot_general(
        anom, y_ref[...], (((1,), (1,)), ((), ())), preferred_element_type=jnp.float32
    ) * (1.0 / (members - 1))
    parts = []
    for lev in range(levs):
        for lat in range(lats):
            weight = loc_ref[lat].astype(jnp.float32)
            for pair in range(pairs):
                at = (lev * share + lat * pairs + pair) * width
                parts.append((cross[at : at + width] * weight).astype(jnp.bfloat16))
    gain = jnp.concatenate(parts, axis=0)
    mean = xbar + jnp.sum(gain.astype(jnp.float32) * w_ref[...], axis=1, keepdims=True)
    update = jnp.dot(gain, z_ref[...], preferred_element_type=jnp.float32)
    result = anom.astype(jnp.float32) - update
    lane = lax.broadcasted_iota(jnp.int32, (width, LANES), 1)
    means = jnp.zeros((width, LANES), jnp.float32)
    for lev in range(levs):
        for lat in range(lats):
            for pair in range(pairs):
                at = (lev * share + lat * pairs + pair) * width
                spot = lat * levs * pairs + lev * pairs + pair
                means = jnp.where(lane == spot, jnp.broadcast_to(mean[at : at + width], (width, LANES)), means)
                for c in range(members // LANES):
                    rows_ref[c, pl.ds(spot, width, stride=stride), :] = result[
                        at : at + width, c * LANES : (c + 1) * LANES
                    ]
    mean_ref[...] = means
    for c in range(members // LANES):
        out_ref[:, c * LANES : (c + 1) * LANES] = rows_ref[c].astype(jnp.bfloat16)


def analyse(relaid, loc, zmat, wvec, ybf):
    levs, share, x_count, members = relaid.shape
    lats, n = loc.shape[1], ybf.shape[0]
    planes = levs * share
    width = min(32, x_count)
    means, out = pl.pallas_call(
        analyse_kernel,
        name="analyse",
        grid=(x_count // width,),
        out_shape=(
            jax.ShapeDtypeStruct((x_count, LANES), jnp.float32),
            jax.ShapeDtypeStruct((x_count * planes, members), jnp.bfloat16),
        ),
        in_specs=[
            pl.BlockSpec((levs, share, width, members), lambda i: (0, 0, i, 0)),
            pl.BlockSpec((lats, width, n), lambda i: (0, i, 0)),
            pl.BlockSpec((n, members), lambda i: (0, 0)),
            pl.BlockSpec((n, members), lambda i: (0, 0)),
            pl.BlockSpec((1, n), lambda i: (0, 0)),
        ],
        out_specs=(
            pl.BlockSpec((width, LANES), lambda i: (i, 0)),
            pl.BlockSpec((width * planes, members), lambda i: (i, 0)),
        ),
        scratch_shapes=[pltpu.VMEM((members // LANES, width * planes, LANES), jnp.float32)],
        compiler_params=pltpu.CompilerParams(vmem_limit_bytes=48 * 1024 * 1024),
    )(relaid, loc.transpose(1, 0, 2), zmat, ybf, wvec[None, :])
    per_lat = planes // lats
    return (
        means[:, :planes].reshape(x_count, lats, per_lat),
        out.reshape(x_count, lats, per_lat, members),
    )


def local(state, obs_col, obs_row, foot_off, obs_lev, obs_val, obs_err, loc):
    level_groups = lax.axis_size("lev")
    ny_total = loc.shape[1] * lax.axis_size("gy") * level_groups
    x_count, y_count, lev_count, members = state.shape
    code = footprint_code(
        obs_col, obs_row, foot_off, obs_lev, (x_count, y_count, lev_count), ny_total,
        lax.axis_index("gy") * y_count, lax.axis_index("lev") * lev_count,
    )
    planes = state.transpose(1, 2, 0, 3).reshape(y_count * lev_count, x_count, members)
    zmat, wcol, ybf, relaid = analysis_weights(planes, code, obs_val, obs_err)
    return analyse(relaid, loc, zmat, wcol[:, 0], ybf)


def solution(mesh):
    return jax.shard_map(
        local,
        mesh=mesh,
        in_specs=(
            P("gx", "gy", "lev", None),
            P("gx"),
            P("gx"),
            P("gx", None),
            P("gx"),
            P("gx"),
            P("gx"),
            P("gx", ("gy", "lev"), None),
        ),
        out_specs=(P("gx", ("gy", "lev"), None), P("gx", ("gy", "lev"), None, None)),
        check_vma=False,
    )
```

```python
import functools

import jax
import jax.numpy as jnp
from jax import lax
from jax.experimental import pallas as pl
from jax.experimental.pallas import tpu as pltpu
from jax.sharding import PartitionSpec as P

KF = 8
HW = 8
DY = 2
SUB = 8
LANES = 128
BLOCK = 64
PIPE = 2
MESH = pl.DeviceIdType.MESH


def footprint_code(obs_col, obs_row, foot_off, obs_lev, shape, ny_total, y_start, lev_start):
    x_count, y_count, lev_count = shape
    planes = y_count * lev_count
    span = 2 * DY + 1
    shift_x = foot_off // span - HW
    shift_y = foot_off % span - DY
    x_here = obs_col[:, None] + shift_x
    y_here = jnp.clip(obs_row[:, None] + shift_y, 0, ny_total - 1) - y_start
    lev_here = obs_lev[:, None] - lev_start
    inside = (y_here >= 0) & (y_here < y_count) & (lev_here >= 0) & (lev_here < lev_count)
    plane = y_here * lev_count + lev_here
    middle = plane * x_count + x_here
    before = planes * x_count + plane * HW + x_here + HW
    after = planes * (x_count + HW) + plane * HW + x_here - x_count
    spot = jnp.where(x_here < 0, before, jnp.where(x_here < x_count, middle, after))
    return jnp.where(inside, spot, -1)


def lane_cast(value, k):
    return jnp.broadcast_to(value[:, k : k + 1], value.shape)


def row_cast(value, i):
    return jnp.broadcast_to(value[i : i + 1, :], value.shape)


def f32_dot(a, b, dims):
    return lax.dot_general(
        a, b, (dims, ((), ())), precision=lax.Precision.HIGHEST, preferred_element_type=jnp.float32
    )


def split_dot(a, b, dims):
    a_high, b_high = a.astype(jnp.bfloat16), b.astype(jnp.bfloat16)
    a_low = (a - a_high.astype(jnp.float32)).astype(jnp.bfloat16)
    b_low = (b - b_high.astype(jnp.float32)).astype(jnp.bfloat16)

    def dot(left, right):
        return lax.dot_general(left, right, (dims, ((), ())), preferred_element_type=jnp.float32)

    return dot(a_high, b_high) + (dot(a_high, b_low) + dot(a_low, b_high))


def factor_block(w_ref, x_ref, root_err):
    rows = w_ref.shape[0]
    groups = rows // SUB
    w = [w_ref[SUB * g : SUB * (g + 1), :] for g in range(groups)]
    x = [x_ref[SUB * g : SUB * (g + 1), :] for g in range(groups)]
    sub_id = lax.broadcasted_iota(jnp.int32, (SUB, LANES), 0)
    for g in range(groups):
        col = {h: [lane_cast(w[h], SUB * g + m) for m in range(SUB)] for h in range(g, groups)}
        s = {(i, m): row_cast(col[g][m], i) for m in range(SUB) for i in range(m, SUB)}
        wr = [row_cast(w[g], i) for i in range(SUB)]
        xr = [row_cast(x[g], i) for i in range(SUB)]
        inv = []
        for k in range(SUB):
            pivot = s[k, k]
            inv_k = lax.rsqrt(pivot)
            inv.append(inv_k)
            minv_k = 1.0 / (pivot * inv_k + row_cast(root_err[g], k))
            for i in range(k + 1, SUB):
                s[i, k] = s[i, k] * inv_k
            for m in range(k + 1, SUB):
                for i in range(m, SUB):
                    s[i, m] = s[i, m] - s[i, k] * s[m, k]
            wr[k] = wr[k] * inv_k
            xr[k] = xr[k] * minv_k
            for i in range(k + 1, SUB):
                wr[i] = wr[i] - s[i, k] * wr[k]
                xr[i] = xr[i] - s[i, k] * xr[k]
        w_new, x_new = wr[0], xr[0]
        for k in range(1, SUB):
            w_new = jnp.where(sub_id == k, wr[k], w_new)
            x_new = jnp.where(sub_id == k, xr[k], x_new)
        w[g], x[g] = w_new, x_new
        for k in reversed(range(SUB)):
            wr[k] = wr[k] * inv[k]
            xr[k] = xr[k] * inv[k]
            for i in range(k):
                wr[i] = wr[i] - s[k, i] * wr[k]
                xr[i] = xr[i] - s[k, i] * xr[k]
        for h in range(g + 1, groups):
            for m in range(SUB):
                w[h] = w[h] - col[h][m] * wr[m]
                x[h] = x[h] - col[h][m] * xr[m]
    for g in range(groups):
        w_ref[SUB * g : SUB * (g + 1), :] = w[g]
        x_ref[SUB * g : SUB * (g + 1), :] = x[g]


def solve_weights(err_ref, z_ref, w_out_ref, y_ref, a_ref, s_ref, root_ref, w_ref, x_ref, inv_ref, low_ref):
    n, members = y_ref.shape
    blocks = n // BLOCK
    ybf = s_ref[:, :members].astype(jnp.bfloat16)
    y_ref[...] = ybf
    root_ref[...] = jnp.broadcast_to(jnp.sqrt(err_ref[...]), (n, LANES))
    same = lax.broadcasted_iota(jnp.int32, (n, n), 0) == lax.broadcasted_iota(jnp.int32, (n, n), 1)
    a_ref[...] = lax.dot_general(ybf, ybf, (((1,), (1,)), ((), ())), preferred_element_type=jnp.float32) / (members - 1) + jnp.where(same, err_ref[...], 0.0)
    eye_w = lax.broadcasted_iota(jnp.int32, (BLOCK, LANES), 0) + BLOCK == lax.broadcasted_iota(jnp.int32, (BLOCK, LANES), 1)
    eye_x = lax.broadcasted_iota(jnp.int32, (BLOCK, LANES), 0) == lax.broadcasted_iota(jnp.int32, (BLOCK, LANES), 1)

    def load_block(at):
        w_ref[...] = jnp.where(eye_w, 1.0, 0.0)
        w_ref[:, :BLOCK] = a_ref[at : at + BLOCK, at : at + BLOCK]
        x_ref[...] = jnp.where(eye_x, 1.0, 0.0)

    load_block(0)

    def step(k, carry):
        base = pl.multiple_of(k * BLOCK, BLOCK)
        root_err = [root_ref[pl.ds(base + SUB * g, SUB), :] for g in range(BLOCK // SUB)]
        factor_block(w_ref, x_ref, root_err)
        for kk in range(blocks):

            @pl.when(k == kk)
            def _():
                at, end = kk * BLOCK, (kk + 1) * BLOCK
                l_inv = w_ref[:, BLOCK:]
                m_inv = x_ref[:, :BLOCK]
                inv_ref[kk] = l_inv
                s_ref[at:end, :members] = f32_dot(m_inv, s_ref[at:end, :members], ((1,), (0,)))
                s_ref[at:end, members:] = f32_dot(l_inv, s_ref[at:end, members:], ((1,), (0,)))
                if end < n:
                    left = end // LANES * LANES
                    panel = f32_dot(a_ref[left:, at:end], l_inv, ((1,), (1,)))
                    below = panel[end - left :]
                    low_ref[kk, end:, :] = below
                    a_ref[end:, left:] = a_ref[end:, left:] - f32_dot(below, panel, ((1,), (1,)))
                    load_block(end)
                    s_ref[end:, :] = s_ref[end:, :] - split_dot(below, s_ref[at:end, :], ((1,), (0,)))

        return carry

    lax.fori_loop(0, blocks, step, 0)
    for kk in reversed(range(blocks)):
        at, end = kk * BLOCK, (kk + 1) * BLOCK
        right = s_ref[at:end, :]
        if end < n:
            right = right - split_dot(low_ref[kk, end:, :], s_ref[end:, :], ((0,), (0,)))
        s_ref[at:end, :] = f32_dot(inv_ref[kk], right, ((0,), (0,)))
    z_ref[...] = s_ref[:, :members].astype(jnp.bfloat16)
    w_out_ref[...] = s_ref[:, members:]


def analysis_weights_kernel(
    axes, code_ref, state_ref, val_ref, err_ref, z_ref, w_out_ref, y_ref, relaid_ref,
    acc_ref, before_ref, after_ref, zin_ref, ys_ref, hb_ref, half_refs,
    a_ref, s_ref, root_ref, w_ref, x_ref, inv_ref, low_ref, send_sem, recv_sem, own_sem,
):
    gxs, gys, levs = axes
    gx, gy, lev = lax.axis_index("gx"), lax.axis_index("gy"), lax.axis_index("lev")
    n, members = acc_ref.shape
    planes, x_count = state_ref.shape[:2]
    edge, inner = planes * HW, planes * x_count
    share = planes // levs
    right, left = lax.rem(gx + 1, gxs), lax.rem(gx + gxs - 1, gxs)
    levels = [(lax.rem(lev + d, levs)) for d in range(1, levs)]
    lats = [(lax.rem(gy + d, gys)) for d in range(1, gys)]
    barrier = pltpu.get_barrier_semaphore()
    peers = [{"gx": right}, {"gx": left}] + [{"lev": v} for v in levels] + [{"gy": v} for v in lats]
    for peer in peers:
        pl.semaphore_signal(barrier, inc=1, device_id=peer, device_id_type=MESH)
    pl.semaphore_wait(barrier, len(peers))
    count = [0]

    def remote(src, dst, peer):
        i = count[0]
        count[0] += 1
        return pltpu.make_async_remote_copy(
            src_ref=src, dst_ref=dst, send_sem=send_sem.at[i], recv_sem=recv_sem.at[i],
            device_id=peer, device_id_type=MESH,
        )

    halo = [
        remote(state_ref.at[:, x_count - HW :], before_ref, {"gx": right}),
        remote(state_ref.at[:, :HW], after_ref, {"gx": left}),
    ]
    for copy in halo:
        copy.start()
    own = pltpu.make_async_copy(state_ref.at[pl.ds(lev * share, share)], relaid_ref.at[lev], own_sem.at[0])
    own.start()

    def chosen(base, width):
        spot = lax.broadcasted_iota(jnp.int32, (n, width), 1) + base
        hits = jnp.zeros((n, width), jnp.float32)
        for slot in range(KF):
            hits = hits + jnp.where(code_ref[:, slot : slot + 1] == spot, 1.0, 0.0)
        return hits.astype(jnp.bfloat16)

    def flat(ref):
        return ref[...].astype(jnp.float32).reshape(edge, members).astype(jnp.bfloat16)

    acc_ref[...] = jnp.zeros_like(acc_ref)

    batch = 4 if planes % 4 == 0 else 1

    def pick(i, carry):
        rows = state_ref[pl.ds(i * batch, batch)].reshape(batch * x_count, members)
        acc_ref[...] += jnp.dot(
            chosen(i * (batch * x_count), batch * x_count), rows, preferred_element_type=jnp.float32
        )
        return carry

    lax.fori_loop(0, planes // batch, pick, 0)
    sel_before, sel_after = chosen(inner, edge), chosen(inner + edge, edge)
    for copy in halo:
        copy.wait()
    acc_ref[...] += jnp.dot(sel_before, flat(before_ref), preferred_element_type=jnp.float32) + jnp.dot(
        sel_after, flat(after_ref), preferred_element_type=jnp.float32
    )
    base, size = 0, n
    bits = levs.bit_length() - 1
    lanes = [slice(c * members // PIPE, (c + 1) * members // PIPE) for c in range(PIPE)]
    bases, flying = [], [[] for _ in lanes]
    for b in range(bits):
        size //= 2
        bit = lax.rem(lev // (1 << b), 2)
        partner = lev + (1 - 2 * bit) * (1 << b)
        keep, give = base + bit * size, base + (1 - bit) * size
        for c, cols in enumerate(lanes):
            for copy in flying[c]:
                copy.wait()
            if b:
                rows = pl.ds(pl.multiple_of(base, 8), size * 2)
                acc_ref[rows, cols] = acc_ref[rows, cols] + half_refs[b - 1][:, cols]
            copy = remote(
                acc_ref.at[pl.ds(pl.multiple_of(give, 8), size), cols], half_refs[b].at[:, cols], {"lev": partner}
            )
            copy.start()
            flying[c] = [copy]
        base = keep
        bases.append((base, size, partner))
    part = n // (levs * gys)
    for c, cols in enumerate(lanes):
        for copy in flying[c]:
            copy.wait()
        if bits:
            rows = pl.ds(pl.multiple_of(base, 8), size)
            acc_ref[rows, cols] = acc_ref[rows, cols] + half_refs[bits - 1][:, cols]
        flying[c] = [
            remote(
                acc_ref.at[pl.ds(pl.multiple_of(base + lat * part, 8), part), cols],
                zin_ref.at[d, :, cols],
                {"gy": lat},
            )
            for d, lat in enumerate(lats)
        ]
        for copy in flying[c]:
            copy.start()
    for copies in flying:
        for copy in copies:
            copy.wait()
    mine = base + gy * part
    total = acc_ref[pl.ds(pl.multiple_of(mine, 8), part), :]
    for d in range(gys - 1):
        total = total + zin_ref[d]
    hx = total / KF
    hbar = jnp.mean(hx, axis=1, keepdims=True)
    chunk = base // part + gy
    ys_ref[chunk] = (hx - hbar).astype(jnp.bfloat16)
    diagonal = lax.broadcasted_iota(jnp.int32, (part, LANES), 0) == lax.broadcasted_iota(
        jnp.int32, (part, LANES), 1
    )
    row = jnp.sum(jnp.where(diagonal, hbar, 0.0), axis=0, keepdims=True)
    hb_ref[chunk] = jnp.broadcast_to(row, (SUB, LANES))
    copies = []
    for lat in lats:
        copies.append(remote(ys_ref.at[chunk], ys_ref.at[chunk], {"gy": lat}))
        copies.append(remote(hb_ref.at[chunk], hb_ref.at[chunk], {"gy": lat}))
    for copy in copies:
        copy.start()
    for copy in copies:
        copy.wait()
    for start, size, partner in reversed(bases):
        span = pl.ds(start // part, size // part)
        copies = [
            remote(ys_ref.at[span], ys_ref.at[span], {"lev": partner}),
            remote(hb_ref.at[span], hb_ref.at[span], {"lev": partner}),
        ]
        for copy in copies:
            copy.start()
        for copy in copies:
            copy.wait()
    copies = [
        remote(state_ref.at[pl.ds(v * share, share)], relaid_ref.at[lev], {"lev": v}) for v in levels
    ]
    for copy in copies:
        copy.start()
    for c in range(levs * gys):
        s_ref[c * part : (c + 1) * part, :members] = ys_ref[c].astype(jnp.float32)
        center = jnp.sum(
            jnp.where(diagonal, jnp.broadcast_to(hb_ref[c][:1, :], (part, LANES)), 0.0), axis=1, keepdims=True
        )
        s_ref[c * part : (c + 1) * part, members:] = jnp.broadcast_to(
            val_ref[c * part : (c + 1) * part, :] - center, (part, LANES)
        )
    solve_weights(err_ref, z_ref, w_out_ref, y_ref, a_ref, s_ref, root_ref, w_ref, x_ref, inv_ref, low_ref)
    for copy in copies:
        copy.wait()
    own.wait()


def analysis_weights(state, code, values, errors):
    axes = tuple(lax.axis_size(name) for name in ("gx", "gy", "lev"))
    gxs, gys, levs = axes
    planes, x_count, members = state.shape
    n = values.shape[0]
    part = n // (gys * levs)
    bits = levs.bit_length() - 1
    copies = 2 + PIPE * (bits + gys - 1) + 2 * (gys - 1) + 2 * bits + (levs - 1)
    vmem = pl.BlockSpec(memory_space=pltpu.VMEM)
    hbm = pl.BlockSpec(memory_space=pl.ANY)
    return pl.pallas_call(
        functools.partial(analysis_weights_kernel, axes),
        name="analysis_weights",
        out_shape=(
            jax.ShapeDtypeStruct((n, members), jnp.bfloat16),
            jax.ShapeDtypeStruct((n, LANES), jnp.float32),
            jax.ShapeDtypeStruct((n, members), jnp.bfloat16),
            jax.ShapeDtypeStruct((levs, planes // levs, x_count, members), jnp.bfloat16),
        ),
        in_specs=[vmem, vmem, vmem, vmem],
        out_specs=(vmem, vmem, vmem, hbm),
        scratch_shapes=[
            pltpu.VMEM((n, members), jnp.float32),
            pltpu.VMEM((planes, HW, members), jnp.bfloat16),
            pltpu.VMEM((planes, HW, members), jnp.bfloat16),
            pltpu.VMEM((gys - 1, part, members), jnp.float32),
            pltpu.VMEM((gys * levs, part, members), jnp.bfloat16),
            pltpu.VMEM((gys * levs, SUB, LANES), jnp.float32),
            [pltpu.VMEM((n >> (b + 1), members), jnp.float32) for b in range(bits)],
            pltpu.VMEM((n, n), jnp.float32),
            pltpu.VMEM((n, members + LANES), jnp.float32),
            pltpu.VMEM((n, LANES), jnp.float32),
            pltpu.VMEM((BLOCK, LANES), jnp.float32),
            pltpu.VMEM((BLOCK, LANES), jnp.float32),
            pltpu.VMEM((n // BLOCK, BLOCK, BLOCK), jnp.float32),
            pltpu.VMEM((n // BLOCK, n, BLOCK), jnp.float32),
            pltpu.SemaphoreType.DMA((copies,)),
            pltpu.SemaphoreType.DMA((copies,)),
            pltpu.SemaphoreType.DMA((1,)),
        ],
        compiler_params=pltpu.CompilerParams(
            collective_id=0, has_side_effects=True, vmem_limit_bytes=48 * 1024 * 1024
        ),
    )(code, state, values[:, None], errors[:, None])


def analyse_kernel(relaid_ref, loc_ref, z_ref, y_ref, w_ref, mean_ref, out_ref, rows_ref):
    levs, share, width, members = relaid_ref.shape
    lats = loc_ref.shape[0]
    pairs = share // lats
    stride = lats * levs * pairs
    block = relaid_ref[...].reshape(levs * share * width, members).astype(jnp.float32)
    xbar = jnp.mean(block, axis=1, keepdims=True)
    anom = (block - xbar).astype(jnp.bfloat16)
    cross = lax.dot_general(
        anom, y_ref[...], (((1,), (1,)), ((), ())), preferred_element_type=jnp.float32
    ) * (1.0 / (members - 1))
    parts = []
    for lev in range(levs):
        for lat in range(lats):
            weight = loc_ref[lat].astype(jnp.float32)
            for pair in range(pairs):
                at = (lev * share + lat * pairs + pair) * width
                parts.append((cross[at : at + width] * weight).astype(jnp.bfloat16))
    gain = jnp.concatenate(parts, axis=0)
    mean = xbar + jnp.sum(gain.astype(jnp.float32) * w_ref[...], axis=1, keepdims=True)
    update = jnp.dot(gain, z_ref[...], preferred_element_type=jnp.float32)
    result = anom.astype(jnp.float32) - update
    lane = lax.broadcasted_iota(jnp.int32, (width, LANES), 1)
    means = jnp.zeros((width, LANES), jnp.float32)
    for lev in range(levs):
        for lat in range(lats):
            for pair in range(pairs):
                at = (lev * share + lat * pairs + pair) * width
                spot = lat * levs * pairs + lev * pairs + pair
                means = jnp.where(lane == spot, jnp.broadcast_to(mean[at : at + width], (width, LANES)), means)
                for c in range(members // LANES):
                    rows_ref[c, pl.ds(spot, width, stride=stride), :] = result[
                        at : at + width, c * LANES : (c + 1) * LANES
                    ]
    mean_ref[...] = means
    for c in range(members // LANES):
        out_ref[:, c * LANES : (c + 1) * LANES] = rows_ref[c].astype(jnp.bfloat16)


def analyse(relaid, loc, zmat, wvec, ybf):
    levs, share, x_count, members = relaid.shape
    lats, n = loc.shape[1], ybf.shape[0]
    planes = levs * share
    width = min(32, x_count)
    means, out = pl.pallas_call(
        analyse_kernel,
        name="analyse",
        grid=(x_count // width,),
        out_shape=(
            jax.ShapeDtypeStruct((x_count, LANES), jnp.float32),
            jax.ShapeDtypeStruct((x_count * planes, members), jnp.bfloat16),
        ),
        in_specs=[
            pl.BlockSpec((levs, share, width, members), lambda i: (0, 0, i, 0)),
            pl.BlockSpec((lats, width, n), lambda i: (0, i, 0)),
            pl.BlockSpec((n, members), lambda i: (0, 0)),
            pl.BlockSpec((n, members), lambda i: (0, 0)),
            pl.BlockSpec((1, n), lambda i: (0, 0)),
        ],
        out_specs=(
            pl.BlockSpec((width, LANES), lambda i: (i, 0)),
            pl.BlockSpec((width * planes, members), lambda i: (i, 0)),
        ),
        scratch_shapes=[pltpu.VMEM((members // LANES, width * planes, LANES), jnp.float32)],
        compiler_params=pltpu.CompilerParams(vmem_limit_bytes=48 * 1024 * 1024),
    )(relaid, loc.transpose(1, 0, 2), zmat, ybf, wvec[None, :])
    per_lat = planes // lats
    return (
        means[:, :planes].reshape(x_count, lats, per_lat),
        out.reshape(x_count, lats, per_lat, members),
    )


def local(state, obs_col, obs_row, foot_off, obs_lev, obs_val, obs_err, loc):
    level_groups = lax.axis_size("lev")
    ny_total = loc.shape[1] * lax.axis_size("gy") * level_groups
    x_count, y_count, lev_count, members = state.shape
    code = footprint_code(
        obs_col, obs_row, foot_off, obs_lev, (x_count, y_count, lev_count), ny_total,
        lax.axis_index("gy") * y_count, lax.axis_index("lev") * lev_count,
    )
    planes = state.transpose(1, 2, 0, 3).reshape(y_count * lev_count, x_count, members)
    zmat, wcol, ybf, relaid = analysis_weights(planes, code, obs_val, obs_err)
    return analyse(relaid, loc, zmat, wcol[:, 0], ybf)


def solution(mesh):
    return jax.shard_map(
        local,
        mesh=mesh,
        in_specs=(
            P("gx", "gy", "lev", None),
            P("gx"),
            P("gx"),
            P("gx", None),
            P("gx"),
            P("gx"),
            P("gx"),
            P("gx", ("gy", "lev"), None),
        ),
        out_specs=(P("gx", ("gy", "lev"), None), P("gx", ("gy", "lev"), None, None)),
        check_vma=False,
    )
```
